32 devices in a mesh: tm: 32 (over z, y, x, core).
Axes of the slice: x: 2, y: 2, z: 4, core: 2. Of those that a mesh axis runs over, the one named last changes fastest.
Arguments:
- samples: int32 [65536, 128], P('tm'), may hold values from -8 to 7
Outputs:
- spectra: float32 [2, 128, 16384], P(None, None, 'tm')
The draws below stay inside these ranges and needn't reach their ends.
All inputs are finite; a program needn't handle non-finite values.
Results may differ from the reference program's by a relative error of at most 0.0003.
Values may be sent and summed in bfloat16 or wider, within the bound.
A program may use at most 192 MiB of HBM per device.

```python
import jax
import jax.numpy as jnp
from jax import lax

INPUTS = 128
LAGS = 128
TOTAL = 65536


def plant(drawn, stream_key, least, high):
    shape = drawn.shape
    index_at = [jax.random.randint(jax.random.fold_in(stream_key, axis), (), 0, shape[axis]) for axis in range(len(shape))]
    drawn = drawn.at[tuple(index_at)].set(least)
    longest = shape.index(max(shape))
    index_at[longest] = (index_at[longest] + 1) % shape[longest]
    return drawn.at[tuple(index_at)].set(high)


def setup_inputs(seed: int = 0) -> dict:
    keys = jax.random.split(jax.random.key(seed), 2)
    samples = plant(jax.random.randint(keys[0], (TOTAL, INPUTS), -8, 8), jax.random.fold_in(keys[0], 1), -8, 7).astype(jnp.int32)
    return dict(samples=samples)


def reference(samples):
    values = samples.astype(jnp.float32)
    total = values.shape[0]
    width = values.shape[1]
    padded = jnp.concatenate([values, jnp.zeros((LAGS, width), jnp.float32)], axis=0)

    def one_lag(lag):
        window = lax.dynamic_slice(padded, (lag.astype(jnp.int32), jnp.int32(0)), (total, width))
        product = jnp.dot(window.T, values, preferred_element_type=jnp.float32, precision=lax.Precision.HIGHEST)
        return product.reshape(width * width)

    lagged = lax.map(one_lag, jnp.arange(LAGS, dtype=jnp.int32))
    lagged = lagged / (16.0 * total)
    transform = jnp.fft.fft(lagged, axis=0)
    return jnp.stack([jnp.real(transform), jnp.imag(transform)]).astype(jnp.float32)
```

```python
import functools

import jax
import jax.numpy as jnp
import numpy as np
from jax import lax
from jax.experimental import pallas as pl
from jax.experimental.pallas import tpu as pltpu
from jax.sharding import PartitionSpec as P

LAGS = 128
Q = 16
JS = 16
TAUS = LAGS + Q
OUT_ROWS = (LAGS + 1) * JS
TILE = OUT_ROWS // 3
CHUNKS = 4
MESH = pl.DeviceIdType.MESH


def flipped(value, mask):
    out = 0
    bit = 1
    while bit <= 64:
        b = (value // bit) % 2
        out = out + ((b + (1 if mask & bit else 0)) % 2) * bit
        bit *= 2
    return out


def code_levels(limit):
    for m in range(8192, 128, -128):
        steps = [m * e + limit / 2**e for e in range(20)]
        if min(steps) <= 32700:
            return m, int(np.argmin(steps)) + 1


def encoded(value, m, levels):
    size = jnp.abs(value)
    code = size
    for e in range(1, levels):
        code = jnp.minimum(code, size * 0.5**e + float(m * e))
    code = (code + 0.5).astype(jnp.int32)
    return jnp.where(value < 0, -code, code).astype(jnp.int16)


def decoded(code, m, levels):
    code = code.astype(jnp.int32).astype(jnp.float32)
    size = jnp.abs(code)
    value = size
    for e in range(1, levels):
        value = jnp.maximum(value, (size - float(m * e)) * 2.0**e)
    return jnp.where(code < 0, -value, value)


def kernel(n, T, G, mj, iw, samples, perm, out, vbuf, ts, tb, ut, acc, sbuf, rbuf,
           send_v, recv_v, send_t, recv_t, send_h, send_r, recv_r):
    me = lax.axis_index("tm")
    g = me % G
    t = me // G
    core = g % 2
    base = t * G
    rows = samples.shape[0]
    R = rows // Q
    C = G // 2
    half = Q // 4
    m_code, levels = code_levels(rows * G * 64)

    barrier = pltpu.get_barrier_semaphore()

    def greet(device):
        pl.semaphore_signal(barrier, inc=1, device_id=(device,), device_id_type=MESH)

    for k in range(1, G):
        greet(base + flipped(g, k))
    for k in range(1, T):
        greet((t + k) % T * G + g)

    @pl.when(t < T - 1)
    def _():
        greet(base + G)

    for q in range(Q):
        phase = samples[pl.ds(q, R, stride=Q), :].astype(jnp.float32).astype(jnp.bfloat16)
        vbuf[g, q // 2, :, (q % 2) * 128:(q % 2 + 1) * 128] = phase

    feeds = jnp.logical_and(g == 0, t > 0)
    pl.semaphore_wait(barrier, jnp.where(feeds, 2 * G + T - 2, G + T - 2))

    def copy_t(k):
        d = flipped(g, k)
        return pltpu.make_async_remote_copy(
            src_ref=ts.at[d], dst_ref=tb.at[g], send_sem=send_t.at[k], recv_sem=recv_t.at[g],
            device_id=(base + d,), device_id_type=MESH)

    def copy_h(d):
        return pltpu.make_async_remote_copy(
            src_ref=ts.at[d], dst_ref=tb.at[G], send_sem=send_h.at[d], recv_sem=recv_t.at[G],
            device_id=(base - G + d,), device_id_type=MESH)

    def copy_v(slot, d, h, sem):
        part = vbuf.at[slot, pl.ds(h * half, half)]
        return pltpu.make_async_remote_copy(
            src_ref=part, dst_ref=part, send_sem=send_v.at[sem, h],
            recv_sem=recv_v.at[slot, h], device_id=(base + d,), device_id_type=MESH)

    partner = flipped(g, 1)
    relay = C == 4
    sends = []

    def send(*what):
        copy_v(*what).start()
        sends.append(what)

    if relay:
        send(g, flipped(g, 2), 1, 1)
        send(g, flipped(g, 4), 0, 2)

    for q in range(Q):
        turned = lax.dot_general(
            perm[...], vbuf[g, q // 2, :, (q % 2) * 128:(q % 2 + 1) * 128],
            (((1,), (1,)), ((), ())), preferred_element_type=jnp.float32
        ).astype(jnp.bfloat16)
        for d in range(G):
            ts[d, q * JS:(q + 1) * JS, :] = turned[d * JS:(d + 1) * JS, :]

    for k in range(G - 1, 0, -1):
        copy_t(k).start()

    @pl.when(jnp.logical_and(g == 0, t > 0))
    def _():
        for d in range(G):
            copy_h(d).start()

    if relay:
        send(g, flipped(g, 2), 0, 1)
        send(g, flipped(g, 4), 1, 2)
    else:
        for c in range(1, C):
            for h in range(2):
                send(g, flipped(g, 2 * c), h, c)
    for h in range(2):
        send(g, partner, h, 0)

    tb[g] = ts[g]

    @pl.when(t == T - 1)
    def _():
        tb[G] = jnp.zeros(tb.shape[1:], tb.dtype)

    @pl.when(t < T - 1)
    def _():
        pltpu.make_async_copy(tb.at[G], tb.at[G], recv_t.at[G]).wait()

    for k in range(1, G):
        s = flipped(g, k)
        pltpu.make_async_copy(tb.at[s], tb.at[s], recv_t.at[s]).wait()

    def build(d, carry):
        pair = jnp.concatenate([tb[d], tb[d + 1]], axis=1)
        ut[d, 0:Q * JS, :] = tb[d]
        for s in range(1, TAUS // Q):
            ut[d, s * Q * JS:(s + 1) * Q * JS, :] = pair[:, s:s + R]
        return carry

    lax.fori_loop(0, G, build, 0)

    def multiply(d, first):
        weights = vbuf[d].reshape(Q // 2 * R, 256)

        def tile(i, carry):
            r0 = pl.multiple_of(i * TILE, JS)
            left = jnp.concatenate(
                [ut[d, pl.ds(pl.multiple_of(r0 + 2 * JS * e, JS), TILE), :] for e in range(Q // 2)], axis=1)
            part = jnp.dot(left, weights, preferred_element_type=jnp.float32)
            for h in range(2):
                half = part[:, h * 128:(h + 1) * 128]
                if first:
                    acc[h, pl.ds(r0, TILE), :] = half
                else:
                    acc[h, pl.ds(r0, TILE), :] += half
            return carry

        lax.fori_loop(0, OUT_ROWS // TILE, tile, 0)

    def wait_v(s, h):
        part = vbuf.at[s, pl.ds(h * half, half)]
        pltpu.make_async_copy(part, part, recv_v.at[s, h]).wait()

    def wait_both(s):
        wait_v(s, 0)
        wait_v(s, 1)

    multiply(g, True)
    wait_both(partner)
    multiply(partner, False)
    if relay:
        x, y, z = (flipped(g, mask) for mask in (2, 4, 6))
        wait_v(x, 1)
        send(x, y, 1, 3)
        wait_v(y, 0)
        send(y, x, 0, 3)
        send(x, partner, 1, 4)
        send(y, partner, 0, 5)
        wait_v(x, 0)
        send(x, partner, 0, 4)
        wait_v(y, 1)
        send(y, partner, 1, 5)
        multiply(x, False)
        multiply(y, False)
        for mask in (3, 5):
            wait_both(flipped(g, mask))
            multiply(flipped(g, mask), False)
        for h in range(2):
            wait_v(z, h)
            send(z, partner, h, 6)
        multiply(z, False)
        wait_both(flipped(g, 7))
        multiply(flipped(g, 7), False)
    else:
        for c in range(1, C):
            s = flipped(g, 2 * c)
            for h in range(2):
                wait_v(s, h)
                send(s, partner, h, C + c - 1)
            multiply(s, False)
            if c > 1:
                s2 = flipped(g, 2 * (c - 1) + 1)
                wait_both(s2)
                multiply(s2, False)
        if C > 1:
            s2 = flipped(g, 2 * (C - 1) + 1)
            wait_both(s2)
            multiply(s2, False)

    def piece(j):
        full = acc[0, pl.ds(j, LAGS, stride=JS), :] + acc[1, pl.ds(JS + j, LAGS, stride=JS), :]
        if iw == 128:
            return full
        return sum(jnp.where(g % (128 // iw) == h, full[:, h * iw:(h + 1) * iw], 0.0) for h in range(128 // iw))

    def copy_r(k):
        d = (t + k) % T
        return pltpu.make_async_remote_copy(
            src_ref=sbuf.at[d], dst_ref=rbuf.at[t], send_sem=send_r.at[k], recv_sem=recv_r.at[t],
            device_id=(d * G + g,), device_id_type=MESH)

    for k in list(range(1, T)) + [0]:
        d = (t + k) % T
        for m in range(mj):
            if k:
                sbuf[d, m] = encoded(piece(d * mj + m), m_code, levels)
            else:
                out[:, m * iw:(m + 1) * iw] = piece(d * mj + m)
        if k:
            copy_r(k).start()
    for k in range(1, T):
        s = (t + T - k) % T
        pltpu.make_async_copy(rbuf.at[s], rbuf.at[s], recv_r.at[s]).wait()
        for m in range(mj):
            out[:, m * iw:(m + 1) * iw] += decoded(rbuf[s, m], m_code, levels)

    for k in range(1, G):
        copy_t(k).wait_send()

    @pl.when(jnp.logical_and(g == 0, t > 0))
    def _():
        for d in range(G):
            copy_h(d).wait_send()

    for what in sends:
        copy_v(*what).wait_send()
    for k in range(1, T):
        copy_r(k).wait_send()


def other(index, mask):
    out = index
    bit = 1
    while bit <= mask:
        if mask & bit:
            out = out + bit - 2 * bit * ((index // bit) % 2)
        bit *= 2
    return out


def unit(limit):
    step = -(-limit // 32000)
    return step, 32700 // step


def shrunk(x, limit, axis=0):
    step, levels = unit(limit)
    largest = jnp.max(jnp.abs(x), axis=axis)
    scale = (largest * (1.0 / step)).astype(jnp.int32) + 1
    return scale.astype(jnp.int16), float(levels) / scale.astype(jnp.float32)


def whole(code):
    return code.astype(jnp.int32).astype(jnp.float32)


def chip_kernel(n, mj, samples, perm, out, vbuf, ts, tb, ut, acc, hs, hr, su, ru, sz, rz, sc,
                send_v, recv_v, send_h, recv_h, send_u, recv_u, send_z, recv_z):
    me = lax.axis_index("tm")
    core = me % 2
    chip = me // 2
    x = chip % 2
    y = (chip // 2) % 2
    z = chip // 4
    chips = n // 2
    Z = chips // 4
    rows = samples.shape[0]
    R = rows // Q
    L = LAGS // CHUNKS
    half = L * JS // 2
    HL = L // 2
    limits = [2 * rows * 64 * s for s in (1, 2, 4)]
    reach = TAUS // Q

    barrier = pltpu.get_barrier_semaphore()

    def greet(device):
        pl.semaphore_signal(barrier, inc=1, device_id=(device,), device_id_type=MESH)

    along_x = other(me, 2)
    along_y = other(me, 4)
    partner = other(me, 1)
    for device in (partner, along_x, along_y):
        greet(device)
    for k in range(1, Z):
        greet((z + k) % Z * 8 + me % 8)

    @pl.when(chip < chips - 1)
    def _():
        greet(2 * chip + 2)

    leads = jnp.logical_and(core == 0, chip > 0)

    for q in range(0, Q, 2):
        pair = [samples[pl.ds(q + p, reach - 1, stride=Q), :].astype(jnp.float32) for p in range(2)]
        hs[q * (reach - 1):(q + 2) * (reach - 1), :] = jnp.concatenate(pair, axis=0).astype(jnp.bfloat16)
    for q in range(Q):
        phase = samples[pl.ds(q, R, stride=Q), :].astype(jnp.float32).astype(jnp.bfloat16)
        vbuf[core, q // 2, :, (q % 2) * 128:(q % 2 + 1) * 128] = phase

    pl.semaphore_wait(barrier, jnp.where(leads, 4 + Z, 2 + Z))

    def copy_h(k):
        return pltpu.make_async_remote_copy(
            src_ref=hs, dst_ref=hr, send_sem=send_h.at[k], recv_sem=recv_h.at[0],
            device_id=(2 * chip - 2 + k,), device_id_type=MESH)

    @pl.when(leads)
    def _():
        for k in range(2):
            copy_h(k).start()

    def copy_v(k):
        src, dst = ((vbuf.at[core], vbuf.at[core]), (ts.at[1 - core], tb.at[core]))[k]
        return pltpu.make_async_remote_copy(
            src_ref=src, dst_ref=dst, send_sem=send_v.at[k], recv_sem=recv_v.at[k],
            device_id=(partner,), device_id_type=MESH)

    copy_v(0).start()

    def transposed(block):
        return lax.dot_general(perm[...], block, (((1,), (1,)), ((), ())), preferred_element_type=jnp.float32)

    for q in range(Q):
        turned = transposed(vbuf[core, q // 2, :, (q % 2) * 128:(q % 2 + 1) * 128]).astype(jnp.bfloat16)
        for k in range(2):
            for a in range(4):
                r0 = (k * 4 + a) * JS
                ts[k, a, q * JS:(q + 1) * JS, :] = turned[r0:r0 + JS, :]

    copy_v(1).start()
    tb[core] = ts[core]

    @pl.when(chip == chips - 1)
    def _():
        hr[...] = jnp.zeros(hr.shape, hr.dtype)

    @pl.when(chip < chips - 1)
    def _():
        pltpu.make_async_copy(hr, hr, recv_h.at[0]).wait()

    edge = lax.dot_general(
        perm[pl.ds(pl.multiple_of(core * 4 * JS, 4 * JS), 4 * JS), :], hr[...],
        (((1,), (1,)), ((), ())), preferred_element_type=jnp.float32)
    for q in range(Q):
        moved = edge if q == 0 else pltpu.roll(edge, 128 - q * (reach - 1), 1)
        for a in range(4):
            tb[2, a, q * JS:(q + 1) * JS, :] = moved[a * JS:(a + 1) * JS, :].astype(jnp.bfloat16)

    for k in range(2):
        there = (vbuf, tb)[k].at[1 - core]
        pltpu.make_async_copy(there, there, recv_v.at[k]).wait()

    def build(first, last):
        def one(a, carry):
            for d in range(2):
                pair = jnp.concatenate([tb[d, a], tb[d + 1, a]], axis=1)
                for s in range(first, last):
                    ut[a, d, s * Q * JS:(s + 1) * Q * JS, :] = pair[:, s:s + R]
            return carry

        lax.fori_loop(0, 4, one, 0)

    def copy_u(t, k):
        return pltpu.make_async_remote_copy(
            src_ref=su.at[t, k], dst_ref=ru.at[t, k], send_sem=send_u.at[t, k], recv_sem=recv_u.at[t, k],
            device_id=(along_x if k in (0, 1, 5) else along_y,), device_id_type=MESH)

    def send(t, k, values, limit):
        blocks = values.reshape(HL, JS, 128)
        code, scale = shrunk(blocks, limit)
        su[t, k, 0:half, :] = jnp.round(blocks * scale[None]).reshape(half, 128).astype(jnp.int32).astype(jnp.int16)
        su[t, k, half:half + JS, :] = code
        copy_u(t, k).start()

    def received(t, k, limit):
        pltpu.make_async_copy(ru.at[t, k], ru.at[t, k], recv_u.at[t, k]).wait()
        scale = whole(ru[t, k, half:half + JS, :]) * (1.0 / unit(limit)[1])
        blocks = whole(ru[t, k, 0:half, :]).reshape(HL, JS, 128)
        return (blocks * scale[None]).reshape(half, 128)

    def multiply(q, t):
        a = (x, 1 - x)[q % 2] + 2 * (y, 1 - y)[q // 2]
        r0 = t * L * JS
        tall = (L + 1) * JS
        left = jnp.concatenate(
            [ut[a, d, r0 + 2 * JS * e:r0 + 2 * JS * e + tall, :] for d in range(2) for e in range(Q // 2)], axis=1)
        part = jnp.dot(left, vbuf[...].reshape(Q * R, 256), preferred_element_type=jnp.float32)
        full = part[0:L * JS, 0:128] + part[JS:tall, 128:256]
        if q == 3:
            send(t, 0, full[0:half], limits[0])
            send(t, 2, full[half:], limits[0])
        elif q == 1:
            send(t, 1, full[0:half], limits[0])
            acc[q, r0 + half:r0 + 2 * half, :] = full[half:]
        elif q == 2:
            send(t, 3, full[half:], limits[0])
            acc[q, r0:r0 + half, :] = full[0:half]
        else:
            acc[q, r0:r0 + 2 * half, :] = full

    def second(t):
        r0 = t * L * JS
        send(t, 4, acc[2, r0:r0 + half, :] + received(t, 0, limits[0]), limits[1])
        send(t, 5, acc[1, r0 + half:r0 + 2 * half, :] + received(t, 2, limits[0]), limits[1])

    def copy_z(t, k):
        d = (z + k) % Z
        return pltpu.make_async_remote_copy(
            src_ref=sz.at[d, t], dst_ref=rz.at[z, t], send_sem=send_z.at[k, t], recv_sem=recv_z.at[z, t],
            device_id=(d * 8 + me % 8,), device_id_type=MESH)

    def third(t):
        r0 = t * L * JS
        for h in range(2):
            near, far = ((1, 4), (3, 5))[h]
            acc[0, r0 + h * half:r0 + (h + 1) * half, :] += received(t, near, limits[0]) + received(t, far, limits[1])
        code, scale = shrunk(acc[0, r0:r0 + 2 * half, :].reshape(L, JS, 128), limits[2])
        sc[t, 0] = scale
        for k in range(1, Z):
            d = (z + k) % Z
            for m in range(mj):
                j = d * mj + m
                values = acc[0, pl.ds(r0 + j, L, stride=JS), :] * sc[t, 0, pl.ds(j, 1), :]
                sz[d, t, m * L:(m + 1) * L, :] = jnp.round(values).astype(jnp.int32).astype(jnp.int16)
            sz[d, t, mj * L:mj * L + JS, :] = code
            copy_z(t, k).start()
        for m in range(mj):
            out[t * L:(t + 1) * L, m * 128:(m + 1) * 128] = acc[0, pl.ds(r0 + z * mj + m, L, stride=JS), :]

    def fourth(t):
        for k in range(1, Z):
            s = (z + Z - k) % Z
            pltpu.make_async_copy(rz.at[s, t], rz.at[s, t], recv_z.at[s, t]).wait()
            sc[t, k] = whole(rz[s, t, mj * L:mj * L + JS, :]) * (1.0 / unit(limits[2])[1])
            for m in range(mj):
                out[t * L:(t + 1) * L, m * 128:(m + 1) * 128] += (
                    whole(rz[s, t, m * L:(m + 1) * L, :]) * sc[t, k, pl.ds(z * mj + m, 1), :])

    grown = 0
    for t in range(CHUNKS + 2):
        if t < CHUNKS:
            need = -(-((t + 1) * L + Q - 1) // Q)
            build(grown, need)
            grown = need
            for q in (3, 1, 2, 0):
                multiply(q, t)
        if 0 <= t - 1 < CHUNKS:
            second(t - 1)
        if 0 <= t - 2 < CHUNKS:
            third(t - 2)
    for t in range(CHUNKS):
        fourth(t)

    @pl.when(leads)
    def _():
        for k in range(2):
            copy_h(k).wait_send()

    for k in range(2):
        copy_v(k).wait_send()
    for t in range(CHUNKS):
        for k in range(6):
            copy_u(t, k).wait_send()
        for k in range(1, Z):
            copy_z(t, k).wait_send()


def chip_lags(n, samples):
    rows, width = samples.shape
    owned = width * width // n
    mj = owned // width
    Z = n // 8
    R = rows // Q
    L = LAGS // CHUNKS
    perm = np.zeros((width, width), np.float32)
    for core in range(2):
        for a in range(4):
            for d in range(Z):
                for m in range(mj):
                    perm[(core * 4 + a) * JS + d * mj + m, (d * 8 + a * 2 + core) * mj + m] = 1
    tall = L * JS // 2 + JS
    return pl.pallas_call(
        functools.partial(chip_kernel, n, mj),
        out_shape=jax.ShapeDtypeStruct((LAGS, owned), jnp.float32),
        in_specs=[pl.BlockSpec(memory_space=pltpu.VMEM)] * 2,
        out_specs=pl.BlockSpec(memory_space=pltpu.VMEM),
        scratch_shapes=[
            pltpu.VMEM((2, Q // 2, R, 2 * width), jnp.bfloat16),
            pltpu.VMEM((2, 4, Q * JS, R), jnp.bfloat16),
            pltpu.VMEM((3, 4, Q * JS, R), jnp.bfloat16),
            pltpu.VMEM((4, 2, TAUS * JS, R), jnp.bfloat16),
            pltpu.VMEM((3, LAGS * JS, width), jnp.float32),
            pltpu.VMEM((Q * (TAUS // Q - 1), width), jnp.bfloat16),
            pltpu.VMEM((Q * (TAUS // Q - 1), width), jnp.bfloat16),
            pltpu.VMEM((CHUNKS, 6, tall, width), jnp.int16),
            pltpu.VMEM((CHUNKS, 6, tall, width), jnp.int16),
            pltpu.VMEM((Z, CHUNKS, mj * L + JS, width), jnp.int16),
            pltpu.VMEM((Z, CHUNKS, mj * L + JS, width), jnp.int16),
            pltpu.VMEM((CHUNKS, Z, JS, width), jnp.float32),
            pltpu.SemaphoreType.DMA((2,)),
            pltpu.SemaphoreType.DMA((2,)),
            pltpu.SemaphoreType.DMA((2,)),
            pltpu.SemaphoreType.DMA((1,)),
            pltpu.SemaphoreType.DMA((CHUNKS, 6)),
            pltpu.SemaphoreType.DMA((CHUNKS, 6)),
            pltpu.SemaphoreType.DMA((Z, CHUNKS)),
            pltpu.SemaphoreType.DMA((Z, CHUNKS)),
        ],
        compiler_params=pltpu.CompilerParams(has_side_effects=True, collective_id=1, vmem_limit_bytes=56 * 1024 * 1024),
    )(samples, jnp.asarray(perm, jnp.bfloat16))


def gathered_lags(n, samples):
    rows, width = samples.shape
    owned = width * width // n
    mj = max(1, owned // width)
    iw = min(width, owned)
    T = JS // mj
    G = n // T
    R = rows // Q
    perm = np.zeros((G * JS, width), np.float32)
    for d in range(G):
        for s in range(T):
            for m in range(mj):
                perm[d * JS + s * mj + m, (s * G + d) * owned // width + m] = 1
    return pl.pallas_call(
        functools.partial(kernel, n, T, G, mj, iw),
        out_shape=jax.ShapeDtypeStruct((LAGS, owned), jnp.float32),
        in_specs=[pl.BlockSpec(memory_space=pltpu.VMEM)] * 2,
        out_specs=pl.BlockSpec(memory_space=pltpu.VMEM),
        scratch_shapes=[
            pltpu.VMEM((G, Q // 2, R, 2 * width), jnp.bfloat16),
            pltpu.VMEM((G, Q * JS, R), jnp.bfloat16),
            pltpu.VMEM((G + 1, Q * JS, R), jnp.bfloat16),
            pltpu.VMEM((G, TAUS * JS, R), jnp.bfloat16),
            pltpu.VMEM((2, OUT_ROWS, width), jnp.float32),
            pltpu.VMEM((T, mj, LAGS, iw), jnp.int16),
            pltpu.VMEM((T, mj, LAGS, iw), jnp.int16),
            pltpu.SemaphoreType.DMA((G, 2)),
            pltpu.SemaphoreType.DMA((G, 2)),
            pltpu.SemaphoreType.DMA((G,)),
            pltpu.SemaphoreType.DMA((G + 1,)),
            pltpu.SemaphoreType.DMA((G,)),
            pltpu.SemaphoreType.DMA((T,)),
            pltpu.SemaphoreType.DMA((T,)),
        ],
        compiler_params=pltpu.CompilerParams(has_side_effects=True, collective_id=0, vmem_limit_bytes=56 * 1024 * 1024),
    )(samples, jnp.asarray(perm, jnp.bfloat16))


def on_device(n, samples):
    rows, width = samples.shape
    owned = width * width // n
    lags = chip_lags if owned >= width and n % 8 == 0 else gathered_lags
    lagged = lags(n, samples)
    k = np.arange(LAGS)
    angle = 2.0 * np.pi / LAGS * (np.outer(k, k) % LAGS)
    table = np.concatenate([np.cos(angle), -np.sin(angle)]) / (16.0 * rows * n)
    spectra = jnp.dot(
        jnp.asarray(table, jnp.float32), lagged,
        preferred_element_type=jnp.float32, precision=lax.Precision.HIGH)
    return spectra.reshape(2, LAGS, owned)


def solution(mesh):
    return jax.shard_map(
        functools.partial(on_device, mesh.shape["tm"]), mesh=mesh,
        in_specs=(P("tm", None),), out_specs=P(None, None, "tm"), check_vma=False)
```

```python
import functools

import jax
import jax.numpy as jnp
import numpy as np
from jax import lax
from jax.experimental import pallas as pl
from jax.experimental.pallas import tpu as pltpu
from jax.sharding import PartitionSpec as P

LAGS = 128
Q = 16
JS = 16
TAUS = LAGS + Q
OUT_ROWS = (LAGS + 1) * JS
TILE = OUT_ROWS // 3
CHUNKS = (32, 32, 32, 16, 16)
MESH = pl.DeviceIdType.MESH


def flipped(value, mask):
    out = 0
    bit = 1
    while bit <= 64:
        b = (value // bit) % 2
        out = out + ((b + (1 if mask & bit else 0)) % 2) * bit
        bit *= 2
    return out


def code_levels(limit):
    for m in range(8192, 128, -128):
        steps = [m * e + limit / 2**e for e in range(20)]
        if min(steps) <= 32700:
            return m, int(np.argmin(steps)) + 1


def encoded(value, m, levels):
    size = jnp.abs(value)
    code = size
    for e in range(1, levels):
        code = jnp.minimum(code, size * 0.5**e + float(m * e))
    code = (code + 0.5).astype(jnp.int32)
    return jnp.where(value < 0, -code, code).astype(jnp.int16)


def decoded(code, m, levels):
    code = code.astype(jnp.int32).astype(jnp.float32)
    size = jnp.abs(code)
    value = size
    for e in range(1, levels):
        value = jnp.maximum(value, (size - float(m * e)) * 2.0**e)
    return jnp.where(code < 0, -value, value)


def kernel(n, T, G, mj, iw, samples, perm, out, vbuf, ts, tb, ut, acc, sbuf, rbuf,
           send_v, recv_v, send_t, recv_t, send_h, send_r, recv_r):
    me = lax.axis_index("tm")
    g = me % G
    t = me // G
    core = g % 2
    base = t * G
    rows = samples.shape[0]
    R = rows // Q
    C = G // 2
    half = Q // 4
    m_code, levels = code_levels(rows * G * 64)

    barrier = pltpu.get_barrier_semaphore()

    def greet(device):
        pl.semaphore_signal(barrier, inc=1, device_id=(device,), device_id_type=MESH)

    for k in range(1, G):
        greet(base + flipped(g, k))
    for k in range(1, T):
        greet((t + k) % T * G + g)

    @pl.when(t < T - 1)
    def _():
        greet(base + G)

    for q in range(Q):
        phase = samples[pl.ds(q, R, stride=Q), :].astype(jnp.float32).astype(jnp.bfloat16)
        vbuf[g, q // 2, :, (q % 2) * 128:(q % 2 + 1) * 128] = phase

    feeds = jnp.logical_and(g == 0, t > 0)
    pl.semaphore_wait(barrier, jnp.where(feeds, 2 * G + T - 2, G + T - 2))

    def copy_t(k):
        d = flipped(g, k)
        return pltpu.make_async_remote_copy(
            src_ref=ts.at[d], dst_ref=tb.at[g], send_sem=send_t.at[k], recv_sem=recv_t.at[g],
            device_id=(base + d,), device_id_type=MESH)

    def copy_h(d):
        return pltpu.make_async_remote_copy(
            src_ref=ts.at[d], dst_ref=tb.at[G], send_sem=send_h.at[d], recv_sem=recv_t.at[G],
            device_id=(base - G + d,), device_id_type=MESH)

    def copy_v(slot, d, h, sem):
        part = vbuf.at[slot, pl.ds(h * half, half)]
        return pltpu.make_async_remote_copy(
            src_ref=part, dst_ref=part, send_sem=send_v.at[sem, h],
            recv_sem=recv_v.at[slot, h], device_id=(base + d,), device_id_type=MESH)

    partner = flipped(g, 1)
    relay = C == 4
    sends = []

    def send(*what):
        copy_v(*what).start()
        sends.append(what)

    if relay:
        send(g, flipped(g, 2), 1, 1)
        send(g, flipped(g, 4), 0, 2)

    for q in range(Q):
        turned = lax.dot_general(
            perm[...], vbuf[g, q // 2, :, (q % 2) * 128:(q % 2 + 1) * 128],
            (((1,), (1,)), ((), ())), preferred_element_type=jnp.float32
        ).astype(jnp.bfloat16)
        for d in range(G):
            ts[d, q * JS:(q + 1) * JS, :] = turned[d * JS:(d + 1) * JS, :]

    for k in range(G - 1, 0, -1):
        copy_t(k).start()

    @pl.when(jnp.logical_and(g == 0, t > 0))
    def _():
        for d in range(G):
            copy_h(d).start()

    if relay:
        send(g, flipped(g, 2), 0, 1)
        send(g, flipped(g, 4), 1, 2)
    else:
        for c in range(1, C):
            for h in range(2):
                send(g, flipped(g, 2 * c), h, c)
    for h in range(2):
        send(g, partner, h, 0)

    tb[g] = ts[g]

    @pl.when(t == T - 1)
    def _():
        tb[G] = jnp.zeros(tb.shape[1:], tb.dtype)

    @pl.when(t < T - 1)
    def _():
        pltpu.make_async_copy(tb.at[G], tb.at[G], recv_t.at[G]).wait()

    for k in range(1, G):
        s = flipped(g, k)
        pltpu.make_async_copy(tb.at[s], tb.at[s], recv_t.at[s]).wait()

    def build(d, carry):
        pair = jnp.concatenate([tb[d], tb[d + 1]], axis=1)
        ut[d, 0:Q * JS, :] = tb[d]
        for s in range(1, TAUS // Q):
            ut[d, s * Q * JS:(s + 1) * Q * JS, :] = pair[:, s:s + R]
        return carry

    lax.fori_loop(0, G, build, 0)

    def multiply(d, first):
        weights = vbuf[d].reshape(Q // 2 * R, 256)

        def tile(i, carry):
            r0 = pl.multiple_of(i * TILE, JS)
            left = jnp.concatenate(
                [ut[d, pl.ds(pl.multiple_of(r0 + 2 * JS * e, JS), TILE), :] for e in range(Q // 2)], axis=1)
            part = jnp.dot(left, weights, preferred_element_type=jnp.float32)
            for h in range(2):
                half = part[:, h * 128:(h + 1) * 128]
                if first:
                    acc[h, pl.ds(r0, TILE), :] = half
                else:
                    acc[h, pl.ds(r0, TILE), :] += half
            return carry

        lax.fori_loop(0, OUT_ROWS // TILE, tile, 0)

    def wait_v(s, h):
        part = vbuf.at[s, pl.ds(h * half, half)]
        pltpu.make_async_copy(part, part, recv_v.at[s, h]).wait()

    def wait_both(s):
        wait_v(s, 0)
        wait_v(s, 1)

    multiply(g, True)
    wait_both(partner)
    multiply(partner, False)
    if relay:
        x, y, z = (flipped(g, mask) for mask in (2, 4, 6))
        wait_v(x, 1)
        send(x, y, 1, 3)
        wait_v(y, 0)
        send(y, x, 0, 3)
        send(x, partner, 1, 4)
        send(y, partner, 0, 5)
        wait_v(x, 0)
        send(x, partner, 0, 4)
        wait_v(y, 1)
        send(y, partner, 1, 5)
        multiply(x, False)
        multiply(y, False)
        for mask in (3, 5):
            wait_both(flipped(g, mask))
            multiply(flipped(g, mask), False)
        for h in range(2):
            wait_v(z, h)
            send(z, partner, h, 6)
        multiply(z, False)
        wait_both(flipped(g, 7))
        multiply(flipped(g, 7), False)
    else:
        for c in range(1, C):
            s = flipped(g, 2 * c)
            for h in range(2):
                wait_v(s, h)
                send(s, partner, h, C + c - 1)
            multiply(s, False)
            if c > 1:
                s2 = flipped(g, 2 * (c - 1) + 1)
                wait_both(s2)
                multiply(s2, False)
        if C > 1:
            s2 = flipped(g, 2 * (C - 1) + 1)
            wait_both(s2)
            multiply(s2, False)

    def piece(j):
        full = acc[0, pl.ds(j, LAGS, stride=JS), :] + acc[1, pl.ds(JS + j, LAGS, stride=JS), :]
        if iw == 128:
            return full
        return sum(jnp.where(g % (128 // iw) == h, full[:, h * iw:(h + 1) * iw], 0.0) for h in range(128 // iw))

    def copy_r(k):
        d = (t + k) % T
        return pltpu.make_async_remote_copy(
            src_ref=sbuf.at[d], dst_ref=rbuf.at[t], send_sem=send_r.at[k], recv_sem=recv_r.at[t],
            device_id=(d * G + g,), device_id_type=MESH)

    for k in list(range(1, T)) + [0]:
        d = (t + k) % T
        for m in range(mj):
            if k:
                sbuf[d, m] = encoded(piece(d * mj + m), m_code, levels)
            else:
                out[:, m * iw:(m + 1) * iw] = piece(d * mj + m)
        if k:
            copy_r(k).start()
    for k in range(1, T):
        s = (t + T - k) % T
        pltpu.make_async_copy(rbuf.at[s], rbuf.at[s], recv_r.at[s]).wait()
        for m in range(mj):
            out[:, m * iw:(m + 1) * iw] += decoded(rbuf[s, m], m_code, levels)

    for k in range(1, G):
        copy_t(k).wait_send()

    @pl.when(jnp.logical_and(g == 0, t > 0))
    def _():
        for d in range(G):
            copy_h(d).wait_send()

    for what in sends:
        copy_v(*what).wait_send()
    for k in range(1, T):
        copy_r(k).wait_send()


def other(index, mask):
    out = index
    bit = 1
    while bit <= mask:
        if mask & bit:
            out = out + bit - 2 * bit * ((index // bit) % 2)
        bit *= 2
    return out


def unit(limit):
    step = -(-limit // 32000)
    return step, 32700 // step


def shrunk(x, limit, axis=0):
    step, levels = unit(limit)
    largest = jnp.max(jnp.abs(x), axis=axis)
    scale = (largest * (1.0 / step)).astype(jnp.int32) + 1
    return scale.astype(jnp.int16), float(levels) / scale.astype(jnp.float32)


def whole(code):
    return code.astype(jnp.int32).astype(jnp.float32)


def chip_kernel(n, mj, samples, perm, out, sv, vbuf, ts, tb, ut, acc, hs, hr, su, ru, sz, rz, sc,
                load, heard, send_v, recv_v, send_h, recv_h, send_u, recv_u, send_z, recv_z):
    me = lax.axis_index("tm")
    core = me % 2
    chip = me // 2
    x = chip % 2
    y = (chip // 2) % 2
    z = chip // 4
    chips = n // 2
    Z = chips // 4
    rows = samples.shape[0]
    R = rows // Q
    starts = [sum(CHUNKS[:t]) for t in range(len(CHUNKS))]
    rounds = max(2, Z - 2)
    limits = [2 * rows * 64 * s for s in (1, 2, 4)]
    reach = TAUS // Q

    barrier = pltpu.get_barrier_semaphore()

    def greet(device):
        pl.semaphore_signal(barrier, inc=1, device_id=(device,), device_id_type=MESH)

    along_x = other(me, 2)
    along_y = other(me, 4)
    partner = other(me, 1)
    up = me + 8
    down = me - 8

    def near(tell):
        tell(along_x)
        tell(along_y)
        pl.when(z > 0)(lambda: tell(down))
        pl.when(z < Z - 1)(lambda: tell(up))

    around = 2 + jnp.where(z > 0, 1, 0) + jnp.where(z < Z - 1, 1, 0)
    greet(partner)
    near(greet)
    fetch = pltpu.make_async_copy(samples, sv, load.at[0])
    fetch.start()
    fetch.wait()

    for q in range(0, Q, 2):
        pair = [sv[pl.ds(q + p, reach - 1, stride=Q), :].astype(jnp.float32) for p in range(2)]
        hs[0, q * (reach - 1):(q + 2) * (reach - 1), :] = jnp.concatenate(pair, axis=0).astype(jnp.bfloat16)
    for q in range(Q):
        phase = sv[pl.ds(q, R, stride=Q), :].astype(jnp.float32).astype(jnp.bfloat16)
        vbuf[core, q // 2, :, (q % 2) * 128:(q % 2 + 1) * 128] = phase

    pl.semaphore_wait(barrier, around + 1)

    def tell(stage):
        near(lambda device: pl.semaphore_signal(
            heard.at[stage], inc=1, device_id=(device,), device_id_type=MESH))

    tell(0)

    def copy_v(k):
        src, dst = ((hs.at[0], hs.at[1]), (vbuf.at[core], vbuf.at[core]), (ts.at[1 - core], tb.at[core]))[k]
        return pltpu.make_async_remote_copy(
            src_ref=src, dst_ref=dst, send_sem=send_v.at[k], recv_sem=recv_v.at[k],
            device_id=(partner,), device_id_type=MESH)

    @pl.when(core == 0)
    def _():
        copy_v(0).start()

    copy_v(1).start()

    def transposed(block):
        return lax.dot_general(perm[...], block, (((1,), (1,)), ((), ())), preferred_element_type=jnp.float32)

    for q in range(Q):
        turned = transposed(vbuf[core, q // 2, :, (q % 2) * 128:(q % 2 + 1) * 128]).astype(jnp.bfloat16)
        for k in range(2):
            for a in range(4):
                r0 = (k * 4 + a) * JS
                ts[k, a, q * JS:(q + 1) * JS, :] = turned[r0:r0 + JS, :]

    copy_v(2).start()
    tb[core] = ts[core]

    @pl.when(core == 1)
    def _():
        pltpu.make_async_copy(hs.at[1], hs.at[1], recv_v.at[0]).wait()

    def copy_h(k):
        return pltpu.make_async_remote_copy(
            src_ref=hs.at[k], dst_ref=hr, send_sem=send_h.at[k], recv_sem=recv_h.at[0],
            device_id=(me - 2,), device_id_type=MESH)

    for stage in range(rounds):
        pl.semaphore_wait(heard.at[stage], around)
        if stage < rounds - 1:
            tell(stage + 1)

    for k in range(2):
        pl.when(jnp.logical_and(chip > 0, core == k))(copy_h(k).start)

    @pl.when(chip == chips - 1)
    def _():
        hr[...] = jnp.zeros(hr.shape, hr.dtype)

    @pl.when(chip < chips - 1)
    def _():
        pltpu.make_async_copy(hr, hr, recv_h.at[0]).wait()

    edge = lax.dot_general(
        perm[pl.ds(pl.multiple_of(core * 4 * JS, 4 * JS), 4 * JS), :], hr[...],
        (((1,), (1,)), ((), ())), preferred_element_type=jnp.float32)
    for q in range(Q):
        moved = edge if q == 0 else pltpu.roll(edge, 128 - q * (reach - 1), 1)
        for a in range(4):
            tb[2, a, q * JS:(q + 1) * JS, :] = moved[a * JS:(a + 1) * JS, :].astype(jnp.bfloat16)

    for k in range(2):
        there = (vbuf, tb)[k].at[1 - core]
        pltpu.make_async_copy(there, there, recv_v.at[k + 1]).wait()

    def build(first, last):
        def one(a, carry):
            for d in range(2):
                pair = jnp.concatenate([tb[d, a], tb[d + 1, a]], axis=1)
                for s in range(first, last):
                    ut[a, d, s * Q * JS:(s + 1) * Q * JS, :] = pair[:, s:s + R]
            return carry

        lax.fori_loop(0, 4, one, 0)

    def copy_u(t, k):
        rows_u = pl.ds(0, (CHUNKS[t] // 2 + 1) * JS)
        return pltpu.make_async_remote_copy(
            src_ref=su.at[t, k, rows_u], dst_ref=ru.at[t, k, rows_u],
            send_sem=send_u.at[t, k], recv_sem=recv_u.at[t, k],
            device_id=(along_x if k in (0, 1, 5) else along_y,), device_id_type=MESH)

    def send(t, k, values, limit):
        half = CHUNKS[t] * JS // 2
        blocks = values.reshape(CHUNKS[t] // 2, JS, 128)
        code, scale = shrunk(blocks, limit)
        su[t, k, 0:half, :] = jnp.round(blocks * scale[None]).reshape(half, 128).astype(jnp.int32).astype(jnp.int16)
        su[t, k, half:half + JS, :] = code
        copy_u(t, k).start()

    def received(t, k, limit):
        half = CHUNKS[t] * JS // 2
        here = ru.at[t, k, pl.ds(0, half + JS)]
        pltpu.make_async_copy(here, here, recv_u.at[t, k]).wait()
        scale = whole(ru[t, k, half:half + JS, :]) * (1.0 / unit(limit)[1])
        blocks = whole(ru[t, k, 0:half, :]).reshape(CHUNKS[t] // 2, JS, 128)
        return (blocks * scale[None]).reshape(half, 128)

    def rows_of(t, h):
        half = CHUNKS[t] * JS // 2
        return starts[t] * JS + h * half, half

    def multiply(q, t):
        a = (x, 1 - x)[q % 2] + 2 * (y, 1 - y)[q // 2]
        full = []
        for h in range(2):
            r0, half = rows_of(t, h)
            left = jnp.concatenate(
                [ut[a, d, r0 + 2 * JS * e:r0 + 2 * JS * e + half + JS, :] for d in range(2) for e in range(Q // 2)], axis=1)
            part = jnp.dot(left, vbuf[...].reshape(Q * R, 256), preferred_element_type=jnp.float32)
            full.append(part[0:half, 0:128] + part[JS:half + JS, 128:256])
        for h in range(2):
            r0, half = rows_of(t, h)
            if q == 3 or q == h + 1:
                send(t, 2 * h + (0 if q == 3 else 1), full[h], limits[0])
            else:
                acc[q, r0:r0 + half, :] = full[h]

    def second(t):
        for h in range(2):
            r0, half = rows_of(t, h)
            send(t, 4 + h, acc[2 - h, r0:r0 + half, :] + received(t, 2 * h, limits[0]), limits[1])

    def copy_z(t, k):
        d = (z + k) % Z
        rows_z = pl.ds(0, mj * CHUNKS[t] + JS)
        return pltpu.make_async_remote_copy(
            src_ref=sz.at[d, t, rows_z], dst_ref=rz.at[z, t, rows_z],
            send_sem=send_z.at[k, t], recv_sem=recv_z.at[z, t],
            device_id=(d * 8 + me % 8,), device_id_type=MESH)

    def third(t):
        L = CHUNKS[t]
        first = starts[t] * JS
        for h in range(2):
            r0, half = rows_of(t, h)
            acc[0, r0:r0 + half, :] += received(t, 2 * h + 1, limits[0]) + received(t, 4 + h, limits[1])
        code, scale = shrunk(acc[0, first:first + L * JS, :].reshape(L, JS, 128), limits[2])
        sc[t, 0] = scale
        for k in range(1, Z):
            d = (z + k) % Z
            for m in range(mj):
                j = d * mj + m
                values = acc[0, pl.ds(first + j, L, stride=JS), :] * sc[t, 0, pl.ds(j, 1), :]
                sz[d, t, m * L:(m + 1) * L, :] = jnp.round(values).astype(jnp.int32).astype(jnp.int16)
            sz[d, t, mj * L:mj * L + JS, :] = code
            copy_z(t, k).start()
        for m in range(mj):
            out[starts[t]:starts[t] + L, m * 128:(m + 1) * 128] = acc[0, pl.ds(first + z * mj + m, L, stride=JS), :]

    def fourth(t):
        L = CHUNKS[t]
        for k in range(1, Z):
            s = (z + Z - k) % Z
            here = rz.at[s, t, pl.ds(0, mj * L + JS)]
            pltpu.make_async_copy(here, here, recv_z.at[s, t]).wait()
            sc[t, k] = whole(rz[s, t, mj * L:mj * L + JS, :]) * (1.0 / unit(limits[2])[1])
            for m in range(mj):
                out[starts[t]:starts[t] + L, m * 128:(m + 1) * 128] += (
                    whole(rz[s, t, m * L:(m + 1) * L, :]) * sc[t, k, pl.ds(z * mj + m, 1), :])

    grown = 0
    for t in range(len(CHUNKS) + 2):
        if t < len(CHUNKS):
            need = -(-(starts[t] + CHUNKS[t] + Q - 1) // Q)
            build(grown, need)
            grown = need
            for q in (3, 1, 2, 0):
                multiply(q, t)
        if 0 <= t - 1 < len(CHUNKS):
            second(t - 1)
        if 0 <= t - 2 < len(CHUNKS):
            third(t - 2)
    for t in range(len(CHUNKS)):
        fourth(t)

    for k in range(2):
        pl.when(jnp.logical_and(chip > 0, core == k))(copy_h(k).wait_send)

    @pl.when(core == 0)
    def _():
        copy_v(0).wait_send()

    for k in range(1, 3):
        copy_v(k).wait_send()
    for t in range(len(CHUNKS)):
        for k in range(6):
            copy_u(t, k).wait_send()
        for k in range(1, Z):
            copy_z(t, k).wait_send()


def chip_lags(n, samples):
    rows, width = samples.shape
    owned = width * width // n
    mj = owned // width
    Z = n // 8
    R = rows // Q
    T = len(CHUNKS)
    L = max(CHUNKS)
    perm = np.zeros((width, width), np.float32)
    for core in range(2):
        for a in range(4):
            for d in range(Z):
                for m in range(mj):
                    perm[(core * 4 + a) * JS + d * mj + m, (d * 8 + a * 2 + core) * mj + m] = 1
    tall = L * JS // 2 + JS
    return pl.pallas_call(
        functools.partial(chip_kernel, n, mj),
        out_shape=jax.ShapeDtypeStruct((LAGS, owned), jnp.float32),
        in_specs=[pl.BlockSpec(memory_space=pltpu.HBM), pl.BlockSpec(memory_space=pltpu.VMEM)],
        out_specs=pl.BlockSpec(memory_space=pltpu.VMEM),
        scratch_shapes=[
            pltpu.VMEM((rows, width), jnp.int32),
            pltpu.VMEM((2, Q // 2, R, 2 * width), jnp.bfloat16),
            pltpu.VMEM((2, 4, Q * JS, R), jnp.bfloat16),
            pltpu.VMEM((3, 4, Q * JS, R), jnp.bfloat16),
            pltpu.VMEM((4, 2, TAUS * JS, R), jnp.bfloat16),
            pltpu.VMEM((3, LAGS * JS, width), jnp.float32),
            pltpu.VMEM((2, Q * (TAUS // Q - 1), width), jnp.bfloat16),
            pltpu.VMEM((Q * (TAUS // Q - 1), width), jnp.bfloat16),
            pltpu.VMEM((T, 6, tall, width), jnp.int16),
            pltpu.VMEM((T, 6, tall, width), jnp.int16),
            pltpu.VMEM((Z, T, mj * L + JS, width), jnp.int16),
            pltpu.VMEM((Z, T, mj * L + JS, width), jnp.int16),
            pltpu.VMEM((T, Z, JS, width), jnp.float32),
            pltpu.SemaphoreType.DMA((1,)),
            pltpu.SemaphoreType.REGULAR((max(2, Z - 2),)),
            pltpu.SemaphoreType.DMA((3,)),
            pltpu.SemaphoreType.DMA((3,)),
            pltpu.SemaphoreType.DMA((2,)),
            pltpu.SemaphoreType.DMA((1,)),
            pltpu.SemaphoreType.DMA((T, 6)),
            pltpu.SemaphoreType.DMA((T, 6)),
            pltpu.SemaphoreType.DMA((Z, T)),
            pltpu.SemaphoreType.DMA((Z, T)),
        ],
        compiler_params=pltpu.CompilerParams(has_side_effects=True, collective_id=1, vmem_limit_bytes=24 * 1024 * 1024),
    )(samples, jnp.asarray(perm, jnp.bfloat16))


def gathered_lags(n, samples):
    rows, width = samples.shape
    owned = width * width // n
    mj = max(1, owned // width)
    iw = min(width, owned)
    T = JS // mj
    G = n // T
    R = rows // Q
    perm = np.zeros((G * JS, width), np.float32)
    for d in range(G):
        for s in range(T):
            for m in range(mj):
                perm[d * JS + s * mj + m, (s * G + d) * owned // width + m] = 1
    return pl.pallas_call(
        functools.partial(kernel, n, T, G, mj, iw),
        out_shape=jax.ShapeDtypeStruct((LAGS, owned), jnp.float32),
        in_specs=[pl.BlockSpec(memory_space=pltpu.VMEM)] * 2,
        out_specs=pl.BlockSpec(memory_space=pltpu.VMEM),
        scratch_shapes=[
            pltpu.VMEM((G, Q // 2, R, 2 * width), jnp.bfloat16),
            pltpu.VMEM((G, Q * JS, R), jnp.bfloat16),
            pltpu.VMEM((G + 1, Q * JS, R), jnp.bfloat16),
            pltpu.VMEM((G, TAUS * JS, R), jnp.bfloat16),
            pltpu.VMEM((2, OUT_ROWS, width), jnp.float32),
            pltpu.VMEM((T, mj, LAGS, iw), jnp.int16),
            pltpu.VMEM((T, mj, LAGS, iw), jnp.int16),
            pltpu.SemaphoreType.DMA((G, 2)),
            pltpu.SemaphoreType.DMA((G, 2)),
            pltpu.SemaphoreType.DMA((G,)),
            pltpu.SemaphoreType.DMA((G + 1,)),
            pltpu.SemaphoreType.DMA((G,)),
            pltpu.SemaphoreType.DMA((T,)),
            pltpu.SemaphoreType.DMA((T,)),
        ],
        compiler_params=pltpu.CompilerParams(has_side_effects=True, collective_id=0, vmem_limit_bytes=56 * 1024 * 1024),
    )(samples, jnp.asarray(perm, jnp.bfloat16))


def on_device(n, samples):
    rows, width = samples.shape
    owned = width * width // n
    lags = chip_lags if owned >= width and n % 8 == 0 else gathered_lags
    lagged = lags(n, samples)
    k = np.arange(LAGS)
    angle = 2.0 * np.pi / LAGS * (np.outer(k, k) % LAGS)
    table = np.concatenate([np.cos(angle), -np.sin(angle)]) / (16.0 * rows * n)
    spectra = jnp.dot(
        jnp.asarray(table, jnp.float32), lagged,
        preferred_element_type=jnp.float32, precision=lax.Precision.HIGH)
    return spectra.reshape(2, LAGS, owned)


def solution(mesh):
    return jax.shard_map(
        functools.partial(on_device, mesh.shape["tm"]), mesh=mesh,
        in_specs=(P("tm", None),), out_specs=P(None, None, "tm"), check_vma=False)
```

```python
import functools

import jax
import jax.numpy as jnp
import numpy as np
from jax import lax
from jax.experimental import pallas as pl
from jax.experimental.pallas import tpu as pltpu
from jax.sharding import PartitionSpec as P

LAGS = 128
Q = 16
JS = 16
TAUS = LAGS + Q
OUT_ROWS = (LAGS + 1) * JS
TILE = OUT_ROWS // 3
CHUNKS = (32, 32, 32, 32)
MESH = pl.DeviceIdType.MESH


def flipped(value, mask):
    out = 0
    bit = 1
    while bit <= 64:
        b = (value // bit) % 2
        out = out + ((b + (1 if mask & bit else 0)) % 2) * bit
        bit *= 2
    return out


def code_levels(limit):
    for m in range(8192, 128, -128):
        steps = [m * e + limit / 2**e for e in range(20)]
        if min(steps) <= 32700:
            return m, int(np.argmin(steps)) + 1


def encoded(value, m, levels):
    size = jnp.abs(value)
    code = size
    for e in range(1, levels):
        code = jnp.minimum(code, size * 0.5**e + float(m * e))
    code = (code + 0.5).astype(jnp.int32)
    return jnp.where(value < 0, -code, code).astype(jnp.int16)


def decoded(code, m, levels):
    code = code.astype(jnp.int32).astype(jnp.float32)
    size = jnp.abs(code)
    value = size
    for e in range(1, levels):
        value = jnp.maximum(value, (size - float(m * e)) * 2.0**e)
    return jnp.where(code < 0, -value, value)


def kernel(n, T, G, mj, iw, samples, perm, out, vbuf, ts, tb, ut, acc, sbuf, rbuf,
           send_v, recv_v, send_t, recv_t, send_h, send_r, recv_r):
    me = lax.axis_index("tm")
    g = me % G
    t = me // G
    core = g % 2
    base = t * G
    rows = samples.shape[0]
    R = rows // Q
    C = G // 2
    half = Q // 4
    m_code, levels = code_levels(rows * G * 64)

    barrier = pltpu.get_barrier_semaphore()

    def greet(device):
        pl.semaphore_signal(barrier, inc=1, device_id=(device,), device_id_type=MESH)

    for k in range(1, G):
        greet(base + flipped(g, k))
    for k in range(1, T):
        greet((t + k) % T * G + g)

    @pl.when(t < T - 1)
    def _():
        greet(base + G)

    for q in range(Q):
        phase = samples[pl.ds(q, R, stride=Q), :].astype(jnp.float32).astype(jnp.bfloat16)
        vbuf[g, q // 2, :, (q % 2) * 128:(q % 2 + 1) * 128] = phase

    feeds = jnp.logical_and(g == 0, t > 0)
    pl.semaphore_wait(barrier, jnp.where(feeds, 2 * G + T - 2, G + T - 2))

    def copy_t(k):
        d = flipped(g, k)
        return pltpu.make_async_remote_copy(
            src_ref=ts.at[d], dst_ref=tb.at[g], send_sem=send_t.at[k], recv_sem=recv_t.at[g],
            device_id=(base + d,), device_id_type=MESH)

    def copy_h(d):
        return pltpu.make_async_remote_copy(
            src_ref=ts.at[d], dst_ref=tb.at[G], send_sem=send_h.at[d], recv_sem=recv_t.at[G],
            device_id=(base - G + d,), device_id_type=MESH)

    def copy_v(slot, d, h, sem):
        part = vbuf.at[slot, pl.ds(h * half, half)]
        return pltpu.make_async_remote_copy(
            src_ref=part, dst_ref=part, send_sem=send_v.at[sem, h],
            recv_sem=recv_v.at[slot, h], device_id=(base + d,), device_id_type=MESH)

    partner = flipped(g, 1)
    relay = C == 4
    sends = []

    def send(*what):
        copy_v(*what).start()
        sends.append(what)

    if relay:
        send(g, flipped(g, 2), 1, 1)
        send(g, flipped(g, 4), 0, 2)

    for q in range(Q):
        turned = lax.dot_general(
            perm[...], vbuf[g, q // 2, :, (q % 2) * 128:(q % 2 + 1) * 128],
            (((1,), (1,)), ((), ())), preferred_element_type=jnp.float32
        ).astype(jnp.bfloat16)
        for d in range(G):
            ts[d, q * JS:(q + 1) * JS, :] = turned[d * JS:(d + 1) * JS, :]

    for k in range(G - 1, 0, -1):
        copy_t(k).start()

    @pl.when(jnp.logical_and(g == 0, t > 0))
    def _():
        for d in range(G):
            copy_h(d).start()

    if relay:
        send(g, flipped(g, 2), 0, 1)
        send(g, flipped(g, 4), 1, 2)
    else:
        for c in range(1, C):
            for h in range(2):
                send(g, flipped(g, 2 * c), h, c)
    for h in range(2):
        send(g, partner, h, 0)

    tb[g] = ts[g]

    @pl.when(t == T - 1)
    def _():
        tb[G] = jnp.zeros(tb.shape[1:], tb.dtype)

    @pl.when(t < T - 1)
    def _():
        pltpu.make_async_copy(tb.at[G], tb.at[G], recv_t.at[G]).wait()

    for k in range(1, G):
        s = flipped(g, k)
        pltpu.make_async_copy(tb.at[s], tb.at[s], recv_t.at[s]).wait()

    def build(d, carry):
        pair = jnp.concatenate([tb[d], tb[d + 1]], axis=1)
        ut[d, 0:Q * JS, :] = tb[d]
        for s in range(1, TAUS // Q):
            ut[d, s * Q * JS:(s + 1) * Q * JS, :] = pair[:, s:s + R]
        return carry

    lax.fori_loop(0, G, build, 0)

    def multiply(d, first):
        weights = vbuf[d].reshape(Q // 2 * R, 256)

        def tile(i, carry):
            r0 = pl.multiple_of(i * TILE, JS)
            left = jnp.concatenate(
                [ut[d, pl.ds(pl.multiple_of(r0 + 2 * JS * e, JS), TILE), :] for e in range(Q // 2)], axis=1)
            part = jnp.dot(left, weights, preferred_element_type=jnp.float32)
            for h in range(2):
                half = part[:, h * 128:(h + 1) * 128]
                if first:
                    acc[h, pl.ds(r0, TILE), :] = half
                else:
                    acc[h, pl.ds(r0, TILE), :] += half
            return carry

        lax.fori_loop(0, OUT_ROWS // TILE, tile, 0)

    def wait_v(s, h):
        part = vbuf.at[s, pl.ds(h * half, half)]
        pltpu.make_async_copy(part, part, recv_v.at[s, h]).wait()

    def wait_both(s):
        wait_v(s, 0)
        wait_v(s, 1)

    multiply(g, True)
    wait_both(partner)
    multiply(partner, False)
    if relay:
        x, y, z = (flipped(g, mask) for mask in (2, 4, 6))
        wait_v(x, 1)
        send(x, y, 1, 3)
        wait_v(y, 0)
        send(y, x, 0, 3)
        send(x, partner, 1, 4)
        send(y, partner, 0, 5)
        wait_v(x, 0)
        send(x, partner, 0, 4)
        wait_v(y, 1)
        send(y, partner, 1, 5)
        multiply(x, False)
        multiply(y, False)
        for mask in (3, 5):
            wait_both(flipped(g, mask))
            multiply(flipped(g, mask), False)
        for h in range(2):
            wait_v(z, h)
            send(z, partner, h, 6)
        multiply(z, False)
        wait_both(flipped(g, 7))
        multiply(flipped(g, 7), False)
    else:
        for c in range(1, C):
            s = flipped(g, 2 * c)
            for h in range(2):
                wait_v(s, h)
                send(s, partner, h, C + c - 1)
            multiply(s, False)
            if c > 1:
                s2 = flipped(g, 2 * (c - 1) + 1)
                wait_both(s2)
                multiply(s2, False)
        if C > 1:
            s2 = flipped(g, 2 * (C - 1) + 1)
            wait_both(s2)
            multiply(s2, False)

    def piece(j):
        full = acc[0, pl.ds(j, LAGS, stride=JS), :] + acc[1, pl.ds(JS + j, LAGS, stride=JS), :]
        if iw == 128:
            return full
        return sum(jnp.where(g % (128 // iw) == h, full[:, h * iw:(h + 1) * iw], 0.0) for h in range(128 // iw))

    def copy_r(k):
        d = (t + k) % T
        return pltpu.make_async_remote_copy(
            src_ref=sbuf.at[d], dst_ref=rbuf.at[t], send_sem=send_r.at[k], recv_sem=recv_r.at[t],
            device_id=(d * G + g,), device_id_type=MESH)

    for k in list(range(1, T)) + [0]:
        d = (t + k) % T
        for m in range(mj):
            if k:
                sbuf[d, m] = encoded(piece(d * mj + m), m_code, levels)
            else:
                out[:, m * iw:(m + 1) * iw] = piece(d * mj + m)
        if k:
            copy_r(k).start()
    for k in range(1, T):
        s = (t + T - k) % T
        pltpu.make_async_copy(rbuf.at[s], rbuf.at[s], recv_r.at[s]).wait()
        for m in range(mj):
            out[:, m * iw:(m + 1) * iw] += decoded(rbuf[s, m], m_code, levels)

    for k in range(1, G):
        copy_t(k).wait_send()

    @pl.when(jnp.logical_and(g == 0, t > 0))
    def _():
        for d in range(G):
            copy_h(d).wait_send()

    for what in sends:
        copy_v(*what).wait_send()
    for k in range(1, T):
        copy_r(k).wait_send()


def other(index, mask):
    out = index
    bit = 1
    while bit <= mask:
        if mask & bit:
            out = out + bit - 2 * bit * ((index // bit) % 2)
        bit *= 2
    return out


def unit(limit):
    step = -(-limit // 32000)
    return step, 32700 // step


def shrunk(x, limit, axis=0):
    step, levels = unit(limit)
    largest = jnp.max(jnp.abs(x), axis=axis)
    scale = (largest * (1.0 / step)).astype(jnp.int32) + 1
    return scale.astype(jnp.int16), float(levels) / scale.astype(jnp.float32)


def whole(code):
    return code.astype(jnp.int32).astype(jnp.float32)


def chip_kernel(n, mj, samples, perm, out, sv, vbuf, ts, tb, ut, acc, hs, hr, su, ru, sz, rz, sc,
                load, heard, send_v, recv_v, send_h, recv_h, send_u, recv_u, send_z, recv_z):
    me = lax.axis_index("tm")
    core = me % 2
    chip = me // 2
    x = chip % 2
    y = (chip // 2) % 2
    z = chip // 4
    chips = n // 2
    Z = chips // 4
    rows = samples.shape[0]
    R = rows // Q
    starts = [sum(CHUNKS[:t]) for t in range(len(CHUNKS))]
    rounds = max(2, Z - 2)
    limits = [2 * rows * 64 * s for s in (1, 2, 4)]
    reach = TAUS // Q

    barrier = pltpu.get_barrier_semaphore()

    def greet(device):
        pl.semaphore_signal(barrier, inc=1, device_id=(device,), device_id_type=MESH)

    along_x = other(me, 2)
    along_y = other(me, 4)
    partner = other(me, 1)
    up = me + 8
    down = me - 8

    def near(tell):
        tell(along_x)
        tell(along_y)
        pl.when(z > 0)(lambda: tell(down))
        pl.when(z < Z - 1)(lambda: tell(up))

    around = 2 + jnp.where(z > 0, 1, 0) + jnp.where(z < Z - 1, 1, 0)
    greet(partner)
    near(greet)
    fetch = pltpu.make_async_copy(samples, sv, load.at[0])
    fetch.start()
    fetch.wait()

    for q in range(0, Q, 2):
        pair = [sv[pl.ds(q + p, reach - 1, stride=Q), :].astype(jnp.float32) for p in range(2)]
        hs[0, q * (reach - 1):(q + 2) * (reach - 1), :] = jnp.concatenate(pair, axis=0).astype(jnp.bfloat16)
    for q in range(Q):
        phase = sv[pl.ds(q, R, stride=Q), :].astype(jnp.float32).astype(jnp.bfloat16)
        vbuf[core, q // 2, :, (q % 2) * 128:(q % 2 + 1) * 128] = phase

    pl.semaphore_wait(barrier, around + 1)

    def tell(stage):
        near(lambda device: pl.semaphore_signal(
            heard.at[stage], inc=1, device_id=(device,), device_id_type=MESH))

    tell(0)

    def copy_v(k):
        src, dst = ((hs.at[0], hs.at[1]), (vbuf.at[core], vbuf.at[core]), (ts.at[1 - core], tb.at[core]))[k]
        return pltpu.make_async_remote_copy(
            src_ref=src, dst_ref=dst, send_sem=send_v.at[k], recv_sem=recv_v.at[k],
            device_id=(partner,), device_id_type=MESH)

    @pl.when(core == 0)
    def _():
        copy_v(0).start()

    copy_v(1).start()

    def transposed(block):
        return lax.dot_general(perm[...], block, (((1,), (1,)), ((), ())), preferred_element_type=jnp.float32)

    for q in range(Q):
        turned = transposed(vbuf[core, q // 2, :, (q % 2) * 128:(q % 2 + 1) * 128]).astype(jnp.bfloat16)
        for k in range(2):
            for a in range(4):
                r0 = (k * 4 + a) * JS
                ts[k, a, q * JS:(q + 1) * JS, :] = turned[r0:r0 + JS, :]

    copy_v(2).start()
    tb[core] = ts[core]

    @pl.when(core == 1)
    def _():
        pltpu.make_async_copy(hs.at[1], hs.at[1], recv_v.at[0]).wait()

    def copy_h(k):
        return pltpu.make_async_remote_copy(
            src_ref=hs.at[k], dst_ref=hr, send_sem=send_h.at[k], recv_sem=recv_h.at[0],
            device_id=(me - 2,), device_id_type=MESH)

    for stage in range(rounds):
        pl.semaphore_wait(heard.at[stage], around)
        if stage < rounds - 1:
            tell(stage + 1)

    for k in range(2):
        pl.when(jnp.logical_and(chip > 0, core == k))(copy_h(k).start)

    for k in range(2):
        there = (vbuf, tb)[k].at[1 - core]
        pltpu.make_async_copy(there, there, recv_v.at[k + 1]).wait()

    places = [(x, 1 - x)[q % 2] + 2 * (y, 1 - y)[q // 2] for q in range(4)]

    def build(q, d, s):
        if s == 0:
            ut[q, d, 0:Q * JS, :] = tb[d, places[q]]
        else:
            pair = jnp.concatenate([tb[d, places[q]], tb[d + 1, places[q]]], axis=1)
            ut[q, d, s * Q * JS:(s + 1) * Q * JS, :] = pair[:, s:s + R]

    def head():
        @pl.when(chip == chips - 1)
        def _():
            hr[...] = jnp.zeros(hr.shape, hr.dtype)

        @pl.when(chip < chips - 1)
        def _():
            pltpu.make_async_copy(hr, hr, recv_h.at[0]).wait()

        edge = lax.dot_general(
            perm[pl.ds(pl.multiple_of(core * 4 * JS, 4 * JS), 4 * JS), :], hr[...],
            (((1,), (1,)), ((), ())), preferred_element_type=jnp.float32)
        for q in range(Q):
            moved = edge if q == 0 else pltpu.roll(edge, 128 - q * (reach - 1), 1)
            for a in range(4):
                tb[2, a, q * JS:(q + 1) * JS, :] = moved[a * JS:(a + 1) * JS, :].astype(jnp.bfloat16)

    def copy_u(t, k):
        rows_u = pl.ds(0, (CHUNKS[t] // 2 + 1) * JS)
        return pltpu.make_async_remote_copy(
            src_ref=su.at[t, k, rows_u], dst_ref=ru.at[t, k, rows_u],
            send_sem=send_u.at[t, k], recv_sem=recv_u.at[t, k],
            device_id=(along_x if k in (0, 1, 5) else along_y,), device_id_type=MESH)

    def send(t, k, values, limit):
        half = CHUNKS[t] * JS // 2
        blocks = values.reshape(CHUNKS[t] // 2, JS, 128)
        code, scale = shrunk(blocks, limit)
        su[t, k, 0:half, :] = jnp.round(blocks * scale[None]).reshape(half, 128).astype(jnp.int32).astype(jnp.int16)
        su[t, k, half:half + JS, :] = code
        copy_u(t, k).start()

    def received(t, k, limit):
        half = CHUNKS[t] * JS // 2
        here = ru.at[t, k, pl.ds(0, half + JS)]
        pltpu.make_async_copy(here, here, recv_u.at[t, k]).wait()
        scale = whole(ru[t, k, half:half + JS, :]) * (1.0 / unit(limit)[1])
        blocks = whole(ru[t, k, 0:half, :]).reshape(CHUNKS[t] // 2, JS, 128)
        return (blocks * scale[None]).reshape(half, 128)

    def rows_of(t, h):
        half = CHUNKS[t] * JS // 2
        return starts[t] * JS + h * half, half

    def products(q, t, blocks):
        full = []
        for h in range(2):
            r0, half = rows_of(t, h)
            left = jnp.concatenate(
                [ut[q, d, r0 + 2 * JS * e:r0 + 2 * JS * e + half + JS, :] for d in blocks for e in range(Q // 2)], axis=1)
            right = vbuf[blocks[0]:blocks[-1] + 1].reshape(len(blocks) * Q // 2 * R, 256)
            part = jnp.dot(left, right, preferred_element_type=jnp.float32)
            full.append(part[0:half, 0:128] + part[JS:half + JS, 128:256])
        return full

    def keep(k, t, full):
        for h in range(2):
            r0, half = rows_of(t, h)
            acc[k, r0:r0 + half, :] = full[h]

    def copy_z(t, k):
        d = (z + k) % Z
        rows_z = pl.ds(0, mj * CHUNKS[t] + JS)
        return pltpu.make_async_remote_copy(
            src_ref=sz.at[d, t, rows_z], dst_ref=rz.at[z, t, rows_z],
            send_sem=send_z.at[k, t], recv_sem=recv_z.at[z, t],
            device_id=(d * 8 + me % 8,), device_id_type=MESH)

    def third(t):
        L = CHUNKS[t]
        first = starts[t] * JS
        for h in range(2):
            r0, half = rows_of(t, h)
            acc[0, r0:r0 + half, :] += received(t, 2 * h + 1, limits[0]) + received(t, 4 + h, limits[1])
        code, scale = shrunk(acc[0, first:first + L * JS, :].reshape(L, JS, 128), limits[2])
        sc[t, 0] = scale
        for k in range(1, Z):
            d = (z + k) % Z
            for m in range(mj):
                j = d * mj + m
                values = acc[0, pl.ds(first + j, L, stride=JS), :] * sc[t, 0, pl.ds(j, 1), :]
                sz[d, t, m * L:(m + 1) * L, :] = jnp.round(values).astype(jnp.int32).astype(jnp.int16)
            sz[d, t, mj * L:mj * L + JS, :] = code
            copy_z(t, k).start()
        for m in range(mj):
            out[starts[t]:starts[t] + L, m * 128:(m + 1) * 128] = acc[0, pl.ds(first + z * mj + m, L, stride=JS), :]

    def fourth(t):
        L = CHUNKS[t]
        for k in range(1, Z):
            s = (z + Z - k) % Z
            here = rz.at[s, t, pl.ds(0, mj * L + JS)]
            pltpu.make_async_copy(here, here, recv_z.at[s, t]).wait()
            sc[t, k] = whole(rz[s, t, mj * L:mj * L + JS, :]) * (1.0 / unit(limits[2])[1])
            for m in range(mj):
                out[starts[t]:starts[t] + L, m * 128:(m + 1) * 128] += (
                    whole(rz[s, t, m * L:(m + 1) * L, :]) * sc[t, k, pl.ds(z * mj + m, 1), :])

    T = len(CHUNKS)

    def some(pieces, t):
        for piece in pieces[t * len(pieces) // T:(t + 1) * len(pieces) // T]:
            build(*piece)

    shifts = range(reach)
    for s in shifts:
        build(3, 0, s)
    for t in range(T):
        some([(q, 0, s) for q in (1, 2, 0) for s in shifts], t)
        keep(1, t, products(3, t, (0,)))
    head()
    for s in shifts:
        build(3, 1, s)
    needed = [0] + [-(-(starts[t] + CHUNKS[t] + Q - 1) // Q) for t in range(T)]

    def outer(t):
        for q in (1, 2, 0):
            for s in range(needed[t], needed[t + 1]):
                build(q, 1, s)
        full = products(3, t, (1,))
        for h in range(2):
            r0, half = rows_of(t, h)
            send(t, 2 * h, acc[1, r0:r0 + half, :] + full[h], limits[0])

    def beside(t):
        one = products(1, t, (0, 1))
        two = products(2, t, (0, 1))
        send(t, 1, one[0], limits[0])
        send(t, 3, two[1], limits[0])
        for h in range(2):
            r0, half = rows_of(t, h)
            acc[2, r0:r0 + half, :] = (two[0], one[1])[h]

    def second(t):
        for h in range(2):
            r0, half = rows_of(t, h)
            send(t, 4 + h, acc[2, r0:r0 + half, :] + received(t, 2 * h, limits[0]), limits[1])

    for t in range(T + 1):
        if t < T:
            outer(t)
        if t > 0:
            keep(0, t - 1, products(0, t - 1, (0, 1)))
            second(t - 1)
        if t < T:
            beside(t)
        if t > 1:
            third(t - 2)
    third(T - 1)
    for t in range(T):
        fourth(t)

    for k in range(2):
        pl.when(jnp.logical_and(chip > 0, core == k))(copy_h(k).wait_send)

    @pl.when(core == 0)
    def _():
        copy_v(0).wait_send()

    for k in range(1, 3):
        copy_v(k).wait_send()
    for t in range(len(CHUNKS)):
        for k in range(6):
            copy_u(t, k).wait_send()
        for k in range(1, Z):
            copy_z(t, k).wait_send()


def chip_lags(n, samples):
    rows, width = samples.shape
    owned = width * width // n
    mj = owned // width
    Z = n // 8
    R = rows // Q
    T = len(CHUNKS)
    L = max(CHUNKS)
    perm = np.zeros((width, width), np.float32)
    for core in range(2):
        for a in range(4):
            for d in range(Z):
                for m in range(mj):
                    perm[(core * 4 + a) * JS + d * mj + m, (d * 8 + a * 2 + core) * mj + m] = 1
    tall = L * JS // 2 + JS
    return pl.pallas_call(
        functools.partial(chip_kernel, n, mj),
        out_shape=jax.ShapeDtypeStruct((LAGS, owned), jnp.float32),
        in_specs=[pl.BlockSpec(memory_space=pltpu.HBM), pl.BlockSpec(memory_space=pltpu.VMEM)],
        out_specs=pl.BlockSpec(memory_space=pltpu.VMEM),
        scratch_shapes=[
            pltpu.VMEM((rows, width), jnp.int32),
            pltpu.VMEM((2, Q // 2, R, 2 * width), jnp.bfloat16),
            pltpu.VMEM((2, 4, Q * JS, R), jnp.bfloat16),
            pltpu.VMEM((3, 4, Q * JS, R), jnp.bfloat16),
            pltpu.VMEM((4, 2, TAUS * JS, R), jnp.bfloat16),
            pltpu.VMEM((3, LAGS * JS, width), jnp.float32),
            pltpu.VMEM((2, Q * (TAUS // Q - 1), width), jnp.bfloat16),
            pltpu.VMEM((Q * (TAUS // Q - 1), width), jnp.bfloat16),
            pltpu.VMEM((T, 6, tall, width), jnp.int16),
            pltpu.VMEM((T, 6, tall, width), jnp.int16),
            pltpu.VMEM((Z, T, mj * L + JS, width), jnp.int16),
            pltpu.VMEM((Z, T, mj * L + JS, width), jnp.int16),
            pltpu.VMEM((T, Z, JS, width), jnp.float32),
            pltpu.SemaphoreType.DMA((1,)),
            pltpu.SemaphoreType.REGULAR((max(2, Z - 2),)),
            pltpu.SemaphoreType.DMA((3,)),
            pltpu.SemaphoreType.DMA((3,)),
            pltpu.SemaphoreType.DMA((2,)),
            pltpu.SemaphoreType.DMA((1,)),
            pltpu.SemaphoreType.DMA((T, 6)),
            pltpu.SemaphoreType.DMA((T, 6)),
            pltpu.SemaphoreType.DMA((Z, T)),
            pltpu.SemaphoreType.DMA((Z, T)),
        ],
        compiler_params=pltpu.CompilerParams(has_side_effects=True, collective_id=1, vmem_limit_bytes=54016 * 1024),
    )(samples, jnp.asarray(perm, jnp.bfloat16))


def gathered_lags(n, samples):
    rows, width = samples.shape
    owned = width * width // n
    mj = max(1, owned // width)
    iw = min(width, owned)
    T = JS // mj
    G = n // T
    R = rows // Q
    perm = np.zeros((G * JS, width), np.float32)
    for d in range(G):
        for s in range(T):
            for m in range(mj):
                perm[d * JS + s * mj + m, (s * G + d) * owned // width + m] = 1
    return pl.pallas_call(
        functools.partial(kernel, n, T, G, mj, iw),
        out_shape=jax.ShapeDtypeStruct((LAGS, owned), jnp.float32),
        in_specs=[pl.BlockSpec(memory_space=pltpu.VMEM)] * 2,
        out_specs=pl.BlockSpec(memory_space=pltpu.VMEM),
        scratch_shapes=[
            pltpu.VMEM((G, Q // 2, R, 2 * width), jnp.bfloat16),
            pltpu.VMEM((G, Q * JS, R), jnp.bfloat16),
            pltpu.VMEM((G + 1, Q * JS, R), jnp.bfloat16),
            pltpu.VMEM((G, TAUS * JS, R), jnp.bfloat16),
            pltpu.VMEM((2, OUT_ROWS, width), jnp.float32),
            pltpu.VMEM((T, mj, LAGS, iw), jnp.int16),
            pltpu.VMEM((T, mj, LAGS, iw), jnp.int16),
            pltpu.SemaphoreType.DMA((G, 2)),
            pltpu.SemaphoreType.DMA((G, 2)),
            pltpu.SemaphoreType.DMA((G,)),
            pltpu.SemaphoreType.DMA((G + 1,)),
            pltpu.SemaphoreType.DMA((G,)),
            pltpu.SemaphoreType.DMA((T,)),
            pltpu.SemaphoreType.DMA((T,)),
        ],
        compiler_params=pltpu.CompilerParams(has_side_effects=True, collective_id=0, vmem_limit_bytes=56 * 1024 * 1024),
    )(samples, jnp.asarray(perm, jnp.bfloat16))


def on_device(n, samples):
    rows, width = samples.shape
    owned = width * width // n
    lags = chip_lags if owned >= width and n % 8 == 0 else gathered_lags
    lagged = lags(n, samples)
    k = np.arange(LAGS)
    angle = 2.0 * np.pi / LAGS * (np.outer(k, k) % LAGS)
    table = np.concatenate([np.cos(angle), -np.sin(angle)]) / (16.0 * rows * n)
    spectra = jnp.dot(
        jnp.asarray(table, jnp.float32), lagged,
        preferred_element_type=jnp.float32, precision=lax.Precision.HIGH)
    return spectra.reshape(2, LAGS, owned)


def solution(mesh):
    return jax.shard_map(
        functools.partial(on_device, mesh.shape["tm"]), mesh=mesh,
        in_specs=(P("tm", None),), out_specs=P(None, None, "tm"), check_vma=False)
```

```python
import functools

import jax
import jax.numpy as jnp
import numpy as np
from jax import lax
from jax.experimental import pallas as pl
from jax.experimental.pallas import tpu as pltpu
from jax.sharding import PartitionSpec as P

LAGS = 128
Q = 16
JS = 16
TAUS = LAGS + Q
OUT_ROWS = (LAGS + 1) * JS
TILE = OUT_ROWS // 3
CHUNKS = (32, 32, 32, 32)
MESH = pl.DeviceIdType.MESH


def flipped(value, mask):
    out = 0
    bit = 1
    while bit <= 64:
        b = (value // bit) % 2
        out = out + ((b + (1 if mask & bit else 0)) % 2) * bit
        bit *= 2
    return out


def code_levels(limit):
    for m in range(8192, 128, -128):
        steps = [m * e + limit / 2**e for e in range(20)]
        if min(steps) <= 32700:
            return m, int(np.argmin(steps)) + 1


def encoded(value, m, levels):
    size = jnp.abs(value)
    code = size
    for e in range(1, levels):
        code = jnp.minimum(code, size * 0.5**e + float(m * e))
    code = (code + 0.5).astype(jnp.int32)
    return jnp.where(value < 0, -code, code).astype(jnp.int16)


def decoded(code, m, levels):
    code = code.astype(jnp.int32).astype(jnp.float32)
    size = jnp.abs(code)
    value = size
    for e in range(1, levels):
        value = jnp.maximum(value, (size - float(m * e)) * 2.0**e)
    return jnp.where(code < 0, -value, value)


def kernel(n, T, G, mj, iw, samples, perm, out, vbuf, ts, tb, ut, acc, sbuf, rbuf,
           send_v, recv_v, send_t, recv_t, send_h, send_r, recv_r):
    me = lax.axis_index("tm")
    g = me % G
    t = me // G
    core = g % 2
    base = t * G
    rows = samples.shape[0]
    R = rows // Q
    C = G // 2
    half = Q // 4
    m_code, levels = code_levels(rows * G * 64)

    barrier = pltpu.get_barrier_semaphore()

    def greet(device):
        pl.semaphore_signal(barrier, inc=1, device_id=(device,), device_id_type=MESH)

    for k in range(1, G):
        greet(base + flipped(g, k))
    for k in range(1, T):
        greet((t + k) % T * G + g)

    @pl.when(t < T - 1)
    def _():
        greet(base + G)

    for q in range(Q):
        phase = samples[pl.ds(q, R, stride=Q), :].astype(jnp.float32).astype(jnp.bfloat16)
        vbuf[g, q // 2, :, (q % 2) * 128:(q % 2 + 1) * 128] = phase

    feeds = jnp.logical_and(g == 0, t > 0)
    pl.semaphore_wait(barrier, jnp.where(feeds, 2 * G + T - 2, G + T - 2))

    def copy_t(k):
        d = flipped(g, k)
        return pltpu.make_async_remote_copy(
            src_ref=ts.at[d], dst_ref=tb.at[g], send_sem=send_t.at[k], recv_sem=recv_t.at[g],
            device_id=(base + d,), device_id_type=MESH)

    def copy_h(d):
        return pltpu.make_async_remote_copy(
            src_ref=ts.at[d], dst_ref=tb.at[G], send_sem=send_h.at[d], recv_sem=recv_t.at[G],
            device_id=(base - G + d,), device_id_type=MESH)

    def copy_v(slot, d, h, sem):
        part = vbuf.at[slot, pl.ds(h * half, half)]
        return pltpu.make_async_remote_copy(
            src_ref=part, dst_ref=part, send_sem=send_v.at[sem, h],
            recv_sem=recv_v.at[slot, h], device_id=(base + d,), device_id_type=MESH)

    partner = flipped(g, 1)
    relay = C == 4
    sends = []

    def send(*what):
        copy_v(*what).start()
        sends.append(what)

    if relay:
        send(g, flipped(g, 2), 1, 1)
        send(g, flipped(g, 4), 0, 2)

    for q in range(Q):
        turned = lax.dot_general(
            perm[...], vbuf[g, q // 2, :, (q % 2) * 128:(q % 2 + 1) * 128],
            (((1,), (1,)), ((), ())), preferred_element_type=jnp.float32
        ).astype(jnp.bfloat16)
        for d in range(G):
            ts[d, q * JS:(q + 1) * JS, :] = turned[d * JS:(d + 1) * JS, :]

    for k in range(G - 1, 0, -1):
        copy_t(k).start()

    @pl.when(jnp.logical_and(g == 0, t > 0))
    def _():
        for d in range(G):
            copy_h(d).start()

    if relay:
        send(g, flipped(g, 2), 0, 1)
        send(g, flipped(g, 4), 1, 2)
    else:
        for c in range(1, C):
            for h in range(2):
                send(g, flipped(g, 2 * c), h, c)
    for h in range(2):
        send(g, partner, h, 0)

    tb[g] = ts[g]

    @pl.when(t == T - 1)
    def _():
        tb[G] = jnp.zeros(tb.shape[1:], tb.dtype)

    @pl.when(t < T - 1)
    def _():
        pltpu.make_async_copy(tb.at[G], tb.at[G], recv_t.at[G]).wait()

    for k in range(1, G):
        s = flipped(g, k)
        pltpu.make_async_copy(tb.at[s], tb.at[s], recv_t.at[s]).wait()

    def build(d, carry):
        pair = jnp.concatenate([tb[d], tb[d + 1]], axis=1)
        ut[d, 0:Q * JS, :] = tb[d]
        for s in range(1, TAUS // Q):
            ut[d, s * Q * JS:(s + 1) * Q * JS, :] = pair[:, s:s + R]
        return carry

    lax.fori_loop(0, G, build, 0)

    def multiply(d, first):
        weights = vbuf[d].reshape(Q // 2 * R, 256)

        def tile(i, carry):
            r0 = pl.multiple_of(i * TILE, JS)
            left = jnp.concatenate(
                [ut[d, pl.ds(pl.multiple_of(r0 + 2 * JS * e, JS), TILE), :] for e in range(Q // 2)], axis=1)
            part = jnp.dot(left, weights, preferred_element_type=jnp.float32)
            for h in range(2):
                half = part[:, h * 128:(h + 1) * 128]
                if first:
                    acc[h, pl.ds(r0, TILE), :] = half
                else:
                    acc[h, pl.ds(r0, TILE), :] += half
            return carry

        lax.fori_loop(0, OUT_ROWS // TILE, tile, 0)

    def wait_v(s, h):
        part = vbuf.at[s, pl.ds(h * half, half)]
        pltpu.make_async_copy(part, part, recv_v.at[s, h]).wait()

    def wait_both(s):
        wait_v(s, 0)
        wait_v(s, 1)

    multiply(g, True)
    wait_both(partner)
    multiply(partner, False)
    if relay:
        x, y, z = (flipped(g, mask) for mask in (2, 4, 6))
        wait_v(x, 1)
        send(x, y, 1, 3)
        wait_v(y, 0)
        send(y, x, 0, 3)
        send(x, partner, 1, 4)
        send(y, partner, 0, 5)
        wait_v(x, 0)
        send(x, partner, 0, 4)
        wait_v(y, 1)
        send(y, partner, 1, 5)
        multiply(x, False)
        multiply(y, False)
        for mask in (3, 5):
            wait_both(flipped(g, mask))
            multiply(flipped(g, mask), False)
        for h in range(2):
            wait_v(z, h)
            send(z, partner, h, 6)
        multiply(z, False)
        wait_both(flipped(g, 7))
        multiply(flipped(g, 7), False)
    else:
        for c in range(1, C):
            s = flipped(g, 2 * c)
            for h in range(2):
                wait_v(s, h)
                send(s, partner, h, C + c - 1)
            multiply(s, False)
            if c > 1:
                s2 = flipped(g, 2 * (c - 1) + 1)
                wait_both(s2)
                multiply(s2, False)
        if C > 1:
            s2 = flipped(g, 2 * (C - 1) + 1)
            wait_both(s2)
            multiply(s2, False)

    def piece(j):
        full = acc[0, pl.ds(j, LAGS, stride=JS), :] + acc[1, pl.ds(JS + j, LAGS, stride=JS), :]
        if iw == 128:
            return full
        return sum(jnp.where(g % (128 // iw) == h, full[:, h * iw:(h + 1) * iw], 0.0) for h in range(128 // iw))

    def copy_r(k):
        d = (t + k) % T
        return pltpu.make_async_remote_copy(
            src_ref=sbuf.at[d], dst_ref=rbuf.at[t], send_sem=send_r.at[k], recv_sem=recv_r.at[t],
            device_id=(d * G + g,), device_id_type=MESH)

    for k in list(range(1, T)) + [0]:
        d = (t + k) % T
        for m in range(mj):
            if k:
                sbuf[d, m] = encoded(piece(d * mj + m), m_code, levels)
            else:
                out[:, m * iw:(m + 1) * iw] = piece(d * mj + m)
        if k:
            copy_r(k).start()
    for k in range(1, T):
        s = (t + T - k) % T
        pltpu.make_async_copy(rbuf.at[s], rbuf.at[s], recv_r.at[s]).wait()
        for m in range(mj):
            out[:, m * iw:(m + 1) * iw] += decoded(rbuf[s, m], m_code, levels)

    for k in range(1, G):
        copy_t(k).wait_send()

    @pl.when(jnp.logical_and(g == 0, t > 0))
    def _():
        for d in range(G):
            copy_h(d).wait_send()

    for what in sends:
        copy_v(*what).wait_send()
    for k in range(1, T):
        copy_r(k).wait_send()


def other(index, mask):
    out = index
    bit = 1
    while bit <= mask:
        if mask & bit:
            out = out + bit - 2 * bit * ((index // bit) % 2)
        bit *= 2
    return out


def unit(limit):
    step = -(-limit // 32000)
    return step, 32700 // step


def shrunk(x, limit, axis=0):
    step, levels = unit(limit)
    largest = jnp.max(jnp.abs(x), axis=axis)
    scale = (largest * (1.0 / step)).astype(jnp.int32) + 1
    return scale.astype(jnp.int16), float(levels) / scale.astype(jnp.float32)


def whole(code):
    return code.astype(jnp.int32).astype(jnp.float32)


def chip_kernel(n, mj, samples, perm, out, sv, vbuf, ts, tb, ut, acc, hs, hr, su, ru, sz, rz, sc,
                load, heard, send_v, recv_v, send_h, recv_h, send_u, recv_u, send_z, recv_z):
    me = lax.axis_index("tm")
    core = me % 2
    chip = me // 2
    x = chip % 2
    y = (chip // 2) % 2
    z = chip // 4
    chips = n // 2
    Z = chips // 4
    rows = samples.shape[0]
    R = rows // Q
    starts = [sum(CHUNKS[:t]) for t in range(len(CHUNKS))]
    rounds = max(2, Z - 2)
    limits = [2 * rows * 64 * s for s in (1, 2, 4)]
    reach = TAUS // Q

    barrier = pltpu.get_barrier_semaphore()

    def greet(device):
        pl.semaphore_signal(barrier, inc=1, device_id=(device,), device_id_type=MESH)

    along_x = other(me, 2)
    along_y = other(me, 4)
    partner = other(me, 1)
    up = me + 8
    down = me - 8

    def near(tell):
        tell(along_x)
        tell(along_y)
        pl.when(z > 0)(lambda: tell(down))
        pl.when(z < Z - 1)(lambda: tell(up))

    around = 2 + jnp.where(z > 0, 1, 0) + jnp.where(z < Z - 1, 1, 0)
    greet(partner)
    near(greet)
    fetch = pltpu.make_async_copy(samples, sv, load.at[0])
    fetch.start()
    fetch.wait()

    for q in range(0, Q, 2):
        pair = [sv[pl.ds(q + p, reach - 1, stride=Q), :].astype(jnp.float32) for p in range(2)]
        hs[0, q * (reach - 1):(q + 2) * (reach - 1), :] = jnp.concatenate(pair, axis=0).astype(jnp.bfloat16)
    for q in range(Q):
        phase = sv[pl.ds(q, R, stride=Q), :].astype(jnp.float32).astype(jnp.bfloat16)
        vbuf[core, q // 2, :, (q % 2) * 128:(q % 2 + 1) * 128] = phase

    pl.semaphore_wait(barrier, around + 1)

    def tell(stage):
        near(lambda device: pl.semaphore_signal(
            heard.at[stage], inc=1, device_id=(device,), device_id_type=MESH))

    tell(0)

    def copy_v(k):
        src, dst = ((hs.at[0], hs.at[1]), (vbuf.at[core], vbuf.at[core]), (ts.at[1 - core], tb.at[core]))[k]
        return pltpu.make_async_remote_copy(
            src_ref=src, dst_ref=dst, send_sem=send_v.at[k], recv_sem=recv_v.at[k],
            device_id=(partner,), device_id_type=MESH)

    @pl.when(core == 0)
    def _():
        copy_v(0).start()

    copy_v(1).start()

    def transposed(block):
        return lax.dot_general(perm[...], block, (((1,), (1,)), ((), ())), preferred_element_type=jnp.float32)

    for q in range(Q):
        turned = transposed(vbuf[core, q // 2, :, (q % 2) * 128:(q % 2 + 1) * 128]).astype(jnp.bfloat16)
        for k in range(2):
            for a in range(4):
                r0 = (k * 4 + a) * JS
                ts[k, a, q * JS:(q + 1) * JS, :] = turned[r0:r0 + JS, :]

    copy_v(2).start()
    tb[core] = ts[core]

    @pl.when(core == 1)
    def _():
        pltpu.make_async_copy(hs.at[1], hs.at[1], recv_v.at[0]).wait()

    def copy_h(k):
        return pltpu.make_async_remote_copy(
            src_ref=hs.at[k], dst_ref=hr, send_sem=send_h.at[k], recv_sem=recv_h.at[0],
            device_id=(me - 2,), device_id_type=MESH)

    for k in range(2):
        pl.when(jnp.logical_and(x == 1, core == k))(copy_h(k).start)

    for stage in range(rounds):
        pl.semaphore_wait(heard.at[stage], around)
        if stage < rounds - 1:
            tell(stage + 1)

    for k in range(2):
        pl.when(jnp.logical_and(jnp.logical_and(chip > 0, x == 0), core == k))(copy_h(k).start)

    for k in range(2):
        there = (vbuf, tb)[k].at[1 - core]
        pltpu.make_async_copy(there, there, recv_v.at[k + 1]).wait()

    places = [(x, 1 - x)[q % 2] + 2 * (y, 1 - y)[q // 2] for q in range(4)]

    def build(q, d, s):
        if s == 0:
            ut[q, d, 0:Q * JS, :] = tb[d, places[q]]
        else:
            pair = jnp.concatenate([tb[d, places[q]], tb[d + 1, places[q]]], axis=1)
            ut[q, d, s * Q * JS:(s + 1) * Q * JS, :] = pair[:, s:s + R]

    def head():
        @pl.when(chip == chips - 1)
        def _():
            hr[...] = jnp.zeros(hr.shape, hr.dtype)

        @pl.when(chip < chips - 1)
        def _():
            pltpu.make_async_copy(hr, hr, recv_h.at[0]).wait()

        edge = lax.dot_general(
            perm[pl.ds(pl.multiple_of(core * 4 * JS, 4 * JS), 4 * JS), :], hr[...],
            (((1,), (1,)), ((), ())), preferred_element_type=jnp.float32)
        for q in range(Q):
            moved = edge if q == 0 else pltpu.roll(edge, 128 - q * (reach - 1), 1)
            for a in range(4):
                tb[2, a, q * JS:(q + 1) * JS, :] = moved[a * JS:(a + 1) * JS, :].astype(jnp.bfloat16)

    def copy_u(t, k):
        rows_u = pl.ds(0, (CHUNKS[t] // 2 + 1) * JS)
        return pltpu.make_async_remote_copy(
            src_ref=su.at[t, k, rows_u], dst_ref=ru.at[t, k, rows_u],
            send_sem=send_u.at[t, k], recv_sem=recv_u.at[t, k],
            device_id=(along_x if k in (0, 1, 5) else along_y,), device_id_type=MESH)

    def send(t, k, values, limit):
        half = CHUNKS[t] * JS // 2
        blocks = values.reshape(CHUNKS[t] // 2, JS, 128)
        code, scale = shrunk(blocks, limit)
        su[t, k, 0:half, :] = jnp.round(blocks * scale[None]).reshape(half, 128).astype(jnp.int32).astype(jnp.int16)
        su[t, k, half:half + JS, :] = code
        copy_u(t, k).start()

    def received(t, k, limit):
        half = CHUNKS[t] * JS // 2
        here = ru.at[t, k, pl.ds(0, half + JS)]
        pltpu.make_async_copy(here, here, recv_u.at[t, k]).wait()
        scale = whole(ru[t, k, half:half + JS, :]) * (1.0 / unit(limit)[1])
        blocks = whole(ru[t, k, 0:half, :]).reshape(CHUNKS[t] // 2, JS, 128)
        return (blocks * scale[None]).reshape(half, 128)

    def rows_of(t, h):
        half = CHUNKS[t] * JS // 2
        return starts[t] * JS + h * half, half

    def products(q, t, blocks):
        full = []
        for h in range(2):
            r0, half = rows_of(t, h)
            left = jnp.concatenate(
                [ut[q, d, r0 + 2 * JS * e:r0 + 2 * JS * e + half + JS, :] for d in blocks for e in range(Q // 2)], axis=1)
            right = vbuf[blocks[0]:blocks[-1] + 1].reshape(len(blocks) * Q // 2 * R, 256)
            part = jnp.dot(left, right, preferred_element_type=jnp.float32)
            full.append(part[0:half, 0:128] + part[JS:half + JS, 128:256])
        return full

    def keep(k, t, full):
        for h in range(2):
            r0, half = rows_of(t, h)
            acc[k, r0:r0 + half, :] = full[h]

    def copy_z(t, k):
        d = (z + k) % Z
        rows_z = pl.ds(0, mj * CHUNKS[t] + JS)
        return pltpu.make_async_remote_copy(
            src_ref=sz.at[d, t, rows_z], dst_ref=rz.at[z, t, rows_z],
            send_sem=send_z.at[k, t], recv_sem=recv_z.at[z, t],
            device_id=(d * 8 + me % 8,), device_id_type=MESH)

    def third(t):
        L = CHUNKS[t]
        first = starts[t] * JS
        for h in range(2):
            r0, half = rows_of(t, h)
            acc[0, r0:r0 + half, :] += received(t, 2 * h + 1, limits[0]) + received(t, 4 + h, limits[1])
        code, scale = shrunk(acc[0, first:first + L * JS, :].reshape(L, JS, 128), limits[2])
        sc[t, 0] = scale
        for k in range(1, Z):
            d = (z + k) % Z
            for m in range(mj):
                j = d * mj + m
                values = acc[0, pl.ds(first + j, L, stride=JS), :] * sc[t, 0, pl.ds(j, 1), :]
                sz[d, t, m * L:(m + 1) * L, :] = jnp.round(values).astype(jnp.int32).astype(jnp.int16)
            sz[d, t, mj * L:mj * L + JS, :] = code
            copy_z(t, k).start()
        for m in range(mj):
            out[starts[t]:starts[t] + L, m * 128:(m + 1) * 128] = acc[0, pl.ds(first + z * mj + m, L, stride=JS), :]

    def fourth(t):
        L = CHUNKS[t]
        for k in range(1, Z):
            s = (z + Z - k) % Z
            here = rz.at[s, t, pl.ds(0, mj * L + JS)]
            pltpu.make_async_copy(here, here, recv_z.at[s, t]).wait()
            sc[t, k] = whole(rz[s, t, mj * L:mj * L + JS, :]) * (1.0 / unit(limits[2])[1])
            for m in range(mj):
                out[starts[t]:starts[t] + L, m * 128:(m + 1) * 128] += (
                    whole(rz[s, t, m * L:(m + 1) * L, :]) * sc[t, k, pl.ds(z * mj + m, 1), :])

    T = len(CHUNKS)

    def some(pieces, t):
        for piece in pieces[t * len(pieces) // T:(t + 1) * len(pieces) // T]:
            build(*piece)

    shifts = range(reach)
    for s in shifts:
        build(3, 0, s)
    for t in range(T):
        some([(q, 0, s) for q in (1, 2, 0) for s in shifts], t)
        keep(1, t, products(3, t, (0,)))
    head()
    needed = [0] + [-(-(starts[t] + CHUNKS[t] + Q - 1) // Q) for t in range(T)]

    def outer(t):
        for q in (3, 1, 2, 0):
            for s in range(needed[t], needed[t + 1]):
                build(q, 1, s)
        full = products(3, t, (1,))
        for h in range(2):
            r0, half = rows_of(t, h)
            send(t, 2 * h, acc[1, r0:r0 + half, :] + full[h], limits[0])

    def beside(t):
        one = products(1, t, (0, 1))
        two = products(2, t, (0, 1))
        send(t, 1, one[0], limits[0])
        send(t, 3, two[1], limits[0])
        for h in range(2):
            r0, half = rows_of(t, h)
            acc[2, r0:r0 + half, :] = (two[0], one[1])[h]

    def second(t):
        for h in range(2):
            r0, half = rows_of(t, h)
            send(t, 4 + h, acc[2, r0:r0 + half, :] + received(t, 2 * h, limits[0]), limits[1])

    for t in range(T + 1):
        if t < T:
            outer(t)
        if t > 0:
            keep(0, t - 1, products(0, t - 1, (0, 1)))
            second(t - 1)
        if t < T:
            beside(t)
        if t > 1:
            third(t - 2)
    third(T - 1)
    for t in range(T):
        fourth(t)

    for k in range(2):
        pl.when(jnp.logical_and(chip > 0, core == k))(copy_h(k).wait_send)

    @pl.when(core == 0)
    def _():
        copy_v(0).wait_send()

    for k in range(1, 3):
        copy_v(k).wait_send()
    for t in range(len(CHUNKS)):
        for k in range(6):
            copy_u(t, k).wait_send()
        for k in range(1, Z):
            copy_z(t, k).wait_send()


def chip_lags(n, samples):
    rows, width = samples.shape
    owned = width * width // n
    mj = owned // width
    Z = n // 8
    R = rows // Q
    T = len(CHUNKS)
    L = max(CHUNKS)
    perm = np.zeros((width, width), np.float32)
    for core in range(2):
        for a in range(4):
            for d in range(Z):
                for m in range(mj):
                    perm[(core * 4 + a) * JS + d * mj + m, (d * 8 + a * 2 + core) * mj + m] = 1
    tall = L * JS // 2 + JS
    return pl.pallas_call(
        functools.partial(chip_kernel, n, mj),
        out_shape=jax.ShapeDtypeStruct((LAGS, owned), jnp.float32),
        in_specs=[pl.BlockSpec(memory_space=pltpu.HBM), pl.BlockSpec(memory_space=pltpu.VMEM)],
        out_specs=pl.BlockSpec(memory_space=pltpu.VMEM),
        scratch_shapes=[
            pltpu.VMEM((rows, width), jnp.int32),
            pltpu.VMEM((2, Q // 2, R, 2 * width), jnp.bfloat16),
            pltpu.VMEM((2, 4, Q * JS, R), jnp.bfloat16),
            pltpu.VMEM((3, 4, Q * JS, R), jnp.bfloat16),
            pltpu.VMEM((4, 2, TAUS * JS, R), jnp.bfloat16),
            pltpu.VMEM((3, LAGS * JS, width), jnp.float32),
            pltpu.VMEM((2, Q * (TAUS // Q - 1), width), jnp.bfloat16),
            pltpu.VMEM((Q * (TAUS // Q - 1), width), jnp.bfloat16),
            pltpu.VMEM((T, 6, tall, width), jnp.int16),
            pltpu.VMEM((T, 6, tall, width), jnp.int16),
            pltpu.VMEM((Z, T, mj * L + JS, width), jnp.int16),
            pltpu.VMEM((Z, T, mj * L + JS, width), jnp.int16),
            pltpu.VMEM((T, Z, JS, width), jnp.float32),
            pltpu.SemaphoreType.DMA((1,)),
            pltpu.SemaphoreType.REGULAR((max(2, Z - 2),)),
            pltpu.SemaphoreType.DMA((3,)),
            pltpu.SemaphoreType.DMA((3,)),
            pltpu.SemaphoreType.DMA((2,)),
            pltpu.SemaphoreType.DMA((1,)),
            pltpu.SemaphoreType.DMA((T, 6)),
            pltpu.SemaphoreType.DMA((T, 6)),
            pltpu.SemaphoreType.DMA((Z, T)),
            pltpu.SemaphoreType.DMA((Z, T)),
        ],
        compiler_params=pltpu.CompilerParams(has_side_effects=True, collective_id=1, vmem_limit_bytes=54016 * 1024),
    )(samples, jnp.asarray(perm, jnp.bfloat16))


def gathered_lags(n, samples):
    rows, width = samples.shape
    owned = width * width // n
    mj = max(1, owned // width)
    iw = min(width, owned)
    T = JS // mj
    G = n // T
    R = rows // Q
    perm = np.zeros((G * JS, width), np.float32)
    for d in range(G):
        for s in range(T):
            for m in range(mj):
                perm[d * JS + s * mj + m, (s * G + d) * owned // width + m] = 1
    return pl.pallas_call(
        functools.partial(kernel, n, T, G, mj, iw),
        out_shape=jax.ShapeDtypeStruct((LAGS, owned), jnp.float32),
        in_specs=[pl.BlockSpec(memory_space=pltpu.VMEM)] * 2,
        out_specs=pl.BlockSpec(memory_space=pltpu.VMEM),
        scratch_shapes=[
            pltpu.VMEM((G, Q // 2, R, 2 * width), jnp.bfloat16),
            pltpu.VMEM((G, Q * JS, R), jnp.bfloat16),
            pltpu.VMEM((G + 1, Q * JS, R), jnp.bfloat16),
            pltpu.VMEM((G, TAUS * JS, R), jnp.bfloat16),
            pltpu.VMEM((2, OUT_ROWS, width), jnp.float32),
            pltpu.VMEM((T, mj, LAGS, iw), jnp.int16),
            pltpu.VMEM((T, mj, LAGS, iw), jnp.int16),
            pltpu.SemaphoreType.DMA((G, 2)),
            pltpu.SemaphoreType.DMA((G, 2)),
            pltpu.SemaphoreType.DMA((G,)),
            pltpu.SemaphoreType.DMA((G + 1,)),
            pltpu.SemaphoreType.DMA((G,)),
            pltpu.SemaphoreType.DMA((T,)),
            pltpu.SemaphoreType.DMA((T,)),
        ],
        compiler_params=pltpu.CompilerParams(has_side_effects=True, collective_id=0, vmem_limit_bytes=56 * 1024 * 1024),
    )(samples, jnp.asarray(perm, jnp.bfloat16))


def on_device(n, samples):
    rows, width = samples.shape
    owned = width * width // n
    lags = chip_lags if owned >= width and n % 8 == 0 else gathered_lags
    lagged = lags(n, samples)
    k = np.arange(LAGS)
    angle = 2.0 * np.pi / LAGS * (np.outer(k, k) % LAGS)
    table = np.concatenate([np.cos(angle), -np.sin(angle)]) / (16.0 * rows * n)
    spectra = jnp.dot(
        jnp.asarray(table, jnp.float32), lagged,
        preferred_element_type=jnp.float32, precision=lax.Precision.HIGH)
    return spectra.reshape(2, LAGS, owned)


def solution(mesh):
    return jax.shard_map(
        functools.partial(on_device, mesh.shape["tm"]), mesh=mesh,
        in_specs=(P("tm", None),), out_specs=P(None, None, "tm"), check_vma=False)
```
